32 devices in a mesh: gx: 4 (over x, core), gy: 2 (over y), gz: 4 (over z).
Axes of the slice: x: 2, y: 2, z: 4, core: 2. Of those that a mesh axis runs over, the one named last changes fastest.
Arguments:
- solution: float32 [16, 8, 16, 256], P(None, 'gx', 'gz', 'gy'), may hold values from -0.6 to 0.6
- residual: float32 [16, 8, 16, 256], P(None, 'gx', 'gz', 'gy'), may hold values from -6 to 6
- direction_prev: float32 [16, 8, 16, 256], P(None, 'gx', 'gz', 'gy'), may hold values from -0.3 to 0.3, as said below
- image_prev: float32 [16, 8, 16, 256], P(None, 'gx', 'gz', 'gy'), may hold values from -9 to 9, as said below
- gram_prev: float32 [16, 16], replicated, may hold values from -32768 to 32768, as said below
Outputs:
- solution_new: float32 [16, 8, 16, 256], P(None, 'gx', 'gz', 'gy')
- residual_new: float32 [16, 8, 16, 256], P(None, 'gx', 'gz', 'gy')
- direction: float32 [16, 8, 16, 256], P(None, 'gx', 'gz', 'gy')
The draws below stay inside these ranges and needn't reach their ends.
Inputs may be any that keep to these rules, and one draw needn't show every extreme that they name: direction_prev is a field of order 0.05. image_prev equals A direction_prev, computed in float32. gram_prev is symmetric and positive definite.
All inputs are finite; a program needn't handle non-finite values.
Results may differ from the reference program's by a relative error of at most 0.0001.
Values sent between devices are 32-bit elements; how exact they have to be, the bound alone decides.
A program may use at most 64 MiB of HBM per device.

```python
import jax
import jax.numpy as jnp
from jax import lax

RHS = 16
NX = 8
NZ = 16
NY = 256


def box_total(padded):
    total = padded[:, :-2] + padded[:, 1:-1] + padded[:, 2:]
    total = total[:, :, :-2] + total[:, :, 1:-1] + total[:, :, 2:]
    return total[:, :, :, :-2] + total[:, :, :, 1:-1] + total[:, :, :, 2:]


def shared_fields(key):
    base = jax.random.fold_in(key, 11)
    shape = (RHS, NX, NZ, NY)
    field = jnp.clip(0.04 * jax.random.normal(base, shape, jnp.float32), -0.24, 0.24)
    padded = jnp.pad(field, ((0, 0), (1, 1), (1, 1), (1, 1)))
    image = 27.0 * field - box_total(padded)
    return (field, image)


def draw_direction_prev(key, part):
    return shared_fields(key)[0]


def draw_image_prev(key, part):
    return shared_fields(key)[1]


def draw_gram_prev(key, part):
    base = jax.random.fold_in(key, 23)
    noise = jax.random.normal(base, (RHS, RHS), jnp.float32)
    matrix = jnp.eye(RHS, dtype=jnp.float32) + 0.05 * (noise + noise.T)
    return matrix * (NX * NY * NZ / 20.0)


def block_scale(key, extent, cuts, smallest, high):
    factor_of, own = 1.0, jax.random.fold_in(key, 6)
    for dim, parts in cuts:
        steps = jnp.exp(jax.random.uniform(jax.random.fold_in(own, dim), (parts,), jnp.float32, smallest / len(cuts), high / len(cuts)))
        factor_of = factor_of * jnp.repeat(steps, extent[dim] // parts).reshape([-1 if axis == dim else 1 for axis in range(len(extent))])
    return factor_of


def gaussian(key, extent, scale, limit, shards=(), kind=jnp.bfloat16):
    level = block_scale(key, extent, shards, -0.22, 0.18) if shards else 1.0
    drawn = jax.random.normal(key, extent, jnp.float32) * scale * level
    return jnp.minimum(jnp.maximum(drawn, -limit), limit).astype(kind)


def setup_inputs(seed: int = 0) -> dict:
    key_of = jax.random.split(jax.random.key(seed), 6)
    return {
        "solution": gaussian(key_of[0], (RHS, NX, NZ, NY), 0.1, 0.6, ((1, 4), (2, 4), (3, 2)), jnp.float32),
        "residual": gaussian(key_of[1], (RHS, NX, NZ, NY), 1.0, 6.0, ((1, 4), (2, 4), (3, 2)), jnp.float32),
        "direction_prev": draw_direction_prev(jax.random.fold_in(key_of[5], 71), 0),
        "image_prev": draw_image_prev(jax.random.fold_in(key_of[5], 71), 0),
        "gram_prev": draw_gram_prev(jax.random.fold_in(key_of[5], 71), 0),
    }


def pad_field(field):
    return jnp.pad(field, ((0, 0), (1, 1), (1, 1), (1, 1)))

def box_sum(padded):
    total = padded[:, :-2] + padded[:, 1:-1] + padded[:, 2:]
    total = total[:, :, :-2] + total[:, :, 1:-1] + total[:, :, 2:]
    return total[:, :, :, :-2] + total[:, :, :, 1:-1] + total[:, :, :, 2:]

def colors_of(shape):
    first = lax.broadcasted_iota(jnp.int32, shape, 1) % 2
    second = lax.broadcasted_iota(jnp.int32, shape, 2) % 2
    third = lax.broadcasted_iota(jnp.int32, shape, 3) % 2
    return 4 * first + 2 * second + third

def gram(left, right):
    return jnp.einsum('kxzy,lxzy->kl', left, right, precision=lax.Precision.HIGHEST)

def combine(field, mixing):
    return jnp.einsum('kxzy,kl->lxzy', field, mixing, precision=lax.Precision.HIGHEST)

def spd_solve(matrix, target):
    order = matrix.shape[0]
    sym = 0.5 * (matrix + matrix.T)
    lower = jnp.zeros_like(sym)
    for col in range(order):
        column = sym[col:, col] - lax.optimization_barrier(jnp.sum(lower[col:, :col] * lower[col, :col][None, :], axis=1))
        pivot = jnp.sqrt(column[0])
        lower = lower.at[col:, col].set(column / pivot)
    middle = jnp.zeros_like(target)
    for row in range(order):
        value = target[row] - lax.optimization_barrier(jnp.sum(lower[row, :row][:, None] * middle[:row], axis=0))
        middle = middle.at[row].set(value / lower[row, row])
    answer = jnp.zeros_like(target)
    for row in range(order - 1, -1, -1):
        value = middle[row] - lax.optimization_barrier(jnp.sum(lower[row + 1:, row][:, None] * answer[row + 1:], axis=0))
        answer = answer.at[row].set(value / lower[row, row])
    return answer

def reference(solution, residual, direction_prev, image_prev, gram_prev):
    colors = colors_of(residual.shape)
    smoothed = jnp.where(colors == 0, residual / 26.0, jnp.float32(0.0))
    for shade in list(range(1, 8)) + list(range(6, -1, -1)):
        boxed = box_sum(pad_field(smoothed))
        smoothed = jnp.where(colors == shade, (residual + boxed - smoothed) / 26.0, smoothed)
    image = 27.0 * smoothed - box_sum(pad_field(smoothed))
    gram_zr = gram(smoothed, residual)
    beta_mix = spd_solve(gram_prev, gram_zr)
    direction = smoothed + combine(direction_prev, beta_mix)
    image_new = image + combine(image_prev, beta_mix)
    curvature = gram(direction, image_new)
    alpha_step = spd_solve(curvature, gram_zr)
    solution_new = solution + combine(direction, alpha_step)
    residual_new = residual - combine(image_new, alpha_step)
    return (solution_new, residual_new, direction)
```

```python
import functools

import jax
import jax.numpy as jnp
from jax import lax
from jax.experimental import pallas as pl
from jax.experimental.pallas import tpu as pltpu
from jax.sharding import PartitionSpec as P


def with_halo(value, sides, width):
    for axis, dim in sides:
        devices, length = (lax.axis_size(axis), value.shape[dim])
        up = [(i, (i + 1) % devices) for i in range(devices - 1)]
        down = [(j, i) for i, j in up]
        last = lax.slice_in_dim(value, length - width, length, axis=dim)
        first = lax.slice_in_dim(value, 0, width, axis=dim)
        before = lax.ppermute(last, axis, up)
        after = lax.ppermute(first, axis, down)
        value = jnp.concatenate([before, value, after], axis=dim)
    return value


def box_sum(padded):
    total = padded[:, :-2] + padded[:, 1:-1] + padded[:, 2:]
    total = total[:, :, :-2] + total[:, :, 1:-1] + total[:, :, 2:]
    return total[:, :, :, :-2] + total[:, :, :, 1:-1] + total[:, :, :, 2:]


def colors_of(shape):
    first = lax.broadcasted_iota(jnp.int32, shape, 1) % 2
    second = lax.broadcasted_iota(jnp.int32, shape, 2) % 2
    third = lax.broadcasted_iota(jnp.int32, shape, 3) % 2
    return 4 * first + 2 * second + third


def local_gram(left, right):
    return jnp.einsum("kxzy,lxzy->kl", left, right, precision=lax.Precision.HIGHEST)


def combine(field, mixing):
    return jnp.einsum("kxzy,kl->lxzy", field, mixing, precision=lax.Precision.HIGHEST)


def small_dot(left, right):
    return jnp.dot(left, right, precision=lax.Precision.HIGHEST)


def spd_solve(matrix, target):
    order = matrix.shape[0]
    sym = 0.5 * (matrix + matrix.T)
    lower = jnp.zeros_like(sym)
    for col in range(order):
        column = sym[col:, col] - jnp.sum(lower[col:, :col] * lower[col, :col][None, :], axis=1)
        pivot = jnp.sqrt(column[0])
        lower = lower.at[col:, col].set(column / pivot)
    middle = jnp.zeros_like(target)
    for row in range(order):
        value = target[row] - jnp.sum(lower[row, :row][:, None] * middle[:row], axis=0)
        middle = middle.at[row].set(value / lower[row, row])
    answer = jnp.zeros_like(target)
    for row in range(order - 1, -1, -1):
        value = middle[row] - jnp.sum(lower[row + 1 :, row][:, None] * answer[row + 1 :], axis=0)
        answer = answer.at[row].set(value / lower[row, row])
    return answer


def sweep_box(field):
    padded = with_halo(field, (("gx", 1), ("gy", 3), ("gz", 2)), 1)
    return box_sum(padded)


def body(solution, residual, direction_prev, image_prev, gram_prev):
    colors = colors_of(residual.shape)
    smoothed = jnp.where(colors == 0, residual / 26.0, jnp.float32(0.0))
    for shade in list(range(1, 8)) + list(range(6, -1, -1)):
        boxed = sweep_box(smoothed)
        smoothed = jnp.where(colors == shade, (residual + boxed - smoothed) / 26.0, smoothed)
    padded = with_halo(smoothed, (("gx", 1), ("gy", 3), ("gz", 2)), 1)
    image = 27.0 * smoothed - box_sum(padded)
    sums = (
        local_gram(smoothed, residual),
        local_gram(smoothed, image),
        local_gram(smoothed, image_prev),
        local_gram(direction_prev, image),
        local_gram(direction_prev, image_prev),
    )
    gram_zr, gram_zw, gram_zq, gram_pw, gram_pq = lax.psum(
        (sums[0], sums[1], sums[2], sums[3], sums[4]), ("gx", "gy", "gz")
    )
    beta_mix = spd_solve(gram_prev, gram_zr)
    direction = smoothed + combine(direction_prev, beta_mix)
    image_new = image + combine(image_prev, beta_mix)
    curvature = gram_zw + small_dot(gram_zq, beta_mix) + small_dot(beta_mix.T, gram_pw)
    curvature = curvature + small_dot(small_dot(beta_mix.T, gram_pq), beta_mix)
    alpha_step = spd_solve(curvature, gram_zr)
    solution_new = solution + combine(direction, alpha_step)
    residual_new = residual - combine(image_new, alpha_step)
    return (solution_new, residual_new, direction)


MESH = pl.DeviceIdType.MESH
HIGHEST = lax.Precision.HIGHEST


def dot(left, right):
    return jnp.dot(left, right, precision=HIGHEST, preferred_element_type=jnp.float32)


def dot_nt(left, right):
    return lax.dot_general(
        left, right, (((1,), (1,)), ((), ())), precision=HIGHEST, preferred_element_type=jnp.float32
    )


def eliminate(matrix, target):
    order = matrix.shape[0]
    rows = lax.broadcasted_iota(jnp.int32, matrix.shape, 0)
    columns = [jnp.broadcast_to(matrix[:, k : k + 1], matrix.shape) for k in range(order)]
    scale = jnp.zeros(matrix.shape, jnp.float32)
    for c in range(order):
        inverse = 1.0 / columns[c][c : c + 1, :]
        here = rows == c
        factor = jnp.where(here, 0.0, columns[c] * inverse)
        for k in range(c + 1, order):
            columns[k] = columns[k] - factor * columns[k][c : c + 1, :]
        target = target - factor * target[c : c + 1, :]
        scale = jnp.where(here, inverse, scale)
    return target * scale


def smooth(res, ngx, ngz, gy, width, emit):
    lx, lz = len(res), len(res[0])
    count, ny = res[0][0].shape
    row = lax.broadcasted_iota(jnp.int32, (count, ny), 0)
    lane = lax.broadcasted_iota(jnp.int32, (count, ny), 1)
    even = lane % 2 == 0
    edges = {
        "xp": (row < ngz, ngz, 0),
        "xn": (row >= count - ngz, count - ngz, 0),
        "zp": (row % ngz == 0, 1, 0),
        "zn": (row % ngz == ngz - 1, count - 1, 0),
        "yp": (lane == jnp.where(gy == 0, 0, -1), 1, 1),
        "yn": (lane == jnp.where(gy == 0, -1, width - 1), ny - 1, 1),
    }
    zero = jnp.zeros((count, ny), jnp.float32)
    memo = {}

    def moved(value, kind):
        if value is None:
            return None
        key = (kind, id(value))
        if key not in memo:
            edge, amount, axis = edges[kind]
            memo[key] = (value, jnp.where(edge, zero, pltpu.roll(value, amount, axis)))
        return memo[key][1]

    def add(*values):
        total = None
        for value in values:
            if value is not None:
                total = value if total is None else total + value
        return total

    state = {(x, z): None for x in range(lx) for z in range(lz)}

    def z_pair(x, z):
        before = state[x, z - 1] if z > 0 else moved(state[x, lz - 1], "zp")
        after = state[x, z + 1] if z < lz - 1 else moved(state[x, 0], "zn")
        return add(before, after)

    def neighbours(x, z):
        def line(other):
            return add(state[other, z], z_pair(other, z))

        before = line(x - 1) if x > 0 else moved_line(lx - 1, z, "xp")
        after = line(x + 1) if x < lx - 1 else moved_line(0, z, "xn")
        return add(z_pair(x, z), before, after)

    def moved_line(x, z, kind):
        return moved(add(state[x, z], z_pair(x, z)), kind)

    def y_pair(value):
        return moved(value, "yp") + moved(value, "yn")

    third = jnp.float32(1.0 / 26.0)
    plan = [(0, 0, (0, 1)), (0, 1, (0, 1)), (1, 0, (0, 1)), (1, 1, (0, 1, 0)), (1, 0, (1, 0)), (0, 1, (1, 0)), (0, 0, (1, 0))]
    forward = {}
    for step, (xp, zp, shades) in enumerate(plan):
        fresh = {}
        for x in range(xp, lx, 2):
            for z in range(zp, lz, 2):
                near = neighbours(x, z)
                base = res[x][z] if near is None else res[x][z] + (near + y_pair(near))
                value = state[x, z]
                for turn, shade in enumerate(shades):
                    total = base if value is None else base + y_pair(value)
                    chosen = even if shade == 0 else jnp.logical_not(even)
                    value = jnp.where(chosen, total * third, zero if value is None else value)
                    if turn == 1 and step < 4:
                        forward[x, z] = value
                fresh[x, z] = value
        state.update(fresh)
        emit(step, forward, state)
    image = {}
    for x in range(lx):
        for z in range(lz):
            box = add(state[x, z], neighbours(x, z))
            image[x, z] = 27.0 * state[x, z] - (box + y_pair(box))
    return image


def pack(value):
    rows = value.shape[0] * value.shape[1] // 128
    return jnp.concatenate([value[i : i + rows] for i in range(0, value.shape[0], rows)], axis=1)


def unpack(value, lanes):
    return jnp.concatenate([value[:, i : i + lanes] for i in range(0, value.shape[1], lanes)], axis=0)


def tree_sum(values):
    while len(values) > 1:
        values = [sum(values[i + 1 : i + 2], values[i]) for i in range(0, len(values), 2)]
    return values[0]


def kernel(
    sizes, sol_in, res_in, dir_in, img_in, gram_in, sol_out, res_out, dir_out,
    sol, res, prev, prev_img, gram, land, strip, halo, done, back, part, parts,
    local_sem, send_sem, recv_sem,
):
    ngx, ngy, ngz, n, lx, lz, width = sizes
    s = lx * lz
    half, stretch = s // 2, 5 * s
    gx, gy, gz = lax.axis_index("gx"), lax.axis_index("gy"), lax.axis_index("gz")
    column = gx * ngz + gz
    place = gy * n + column
    everyone = n * ngy

    loads = [
        pltpu.make_async_copy(a, b, local_sem.at[i])
        for i, (a, b) in enumerate(
            ((res_in, res), (gram_in, gram), (dir_in, prev), (img_in, prev_img), (sol_in, sol))
        )
    ]
    for load in loads:
        load.start()

    ways = sorted(
        ((dx, dy, dz) for dx in range(ngx) for dy in range(ngy) for dz in range(ngz)),
        key=lambda way: (-min(way[2], ngz - way[2]), -min(way[0], ngx - way[0]), -way[1]),
    )[:-1]
    flock = []
    for dx, dy, dz in ways:
        ox, oy, oz = lax.rem(gx + dx, ngx), lax.rem(gy + dy, ngy), lax.rem(gz + dz, ngz)
        flock.append((dy == 0, ox * ngz + oz, {"gx": ox, "gy": oy, "gz": oz}))

    def remote(source, target, sent, arrived, where):
        pltpu.make_async_remote_copy(
            src_ref=source, dst_ref=target, send_sem=send_sem.at[sent], recv_sem=recv_sem.at[arrived],
            device_id=where, device_id_type=MESH,
        ).start()

    def wait(ref, semaphore):
        pltpu.make_async_copy(ref, ref, semaphore).wait()

    barrier = pltpu.get_barrier_semaphore()
    for _, _, where in flock:
        pl.semaphore_signal(barrier, inc=1, device_id=where, device_id_type=MESH)
    loads[0].wait()
    depth = width // s
    lanes = lax.broadcasted_iota(jnp.int32, (n, width), 1)
    packed = jnp.zeros((n, width), jnp.float32)
    for i in range(s):
        line = res[pl.ds(i, n, stride=s), :]
        line = pltpu.roll(line, lax.rem(i * depth + jnp.where(gy == 0, depth, 0), width), 1)
        packed = jnp.where(lanes // depth == i, line, packed)
    for i in range(n):
        strip[i] = packed[i : i + 1, :]
    pl.semaphore_wait(barrier, everyone - 1)

    mine = land.at[pl.ds(column * s, s), :]
    for near, oc, where in flock:
        if near:
            remote(res.at[pl.ds(oc * s, s), :], mine, 0, 0, where)
        else:
            remote(strip.at[oc], halo.at[column], 0, 1, where)
    pltpu.make_async_copy(res.at[pl.ds(column * s, s), :], mine, recv_sem.at[0]).start()

    def flat(ref, offsets, stride):
        return jnp.concatenate([ref[pl.ds(i, n, stride=stride), :] for i in offsets], axis=1)

    def place_of(x, z, final):
        slot = x % 2 if final == 0 else 3 - x % 2
        return slot * s + x // 2 * lz + z

    planes = [(x, z) for x in range(lx) for z in range(lz)]
    for load in loads[1:4]:
        load.wait()
    eye = (lax.broadcasted_iota(jnp.int32, (n, n), 0) == lax.broadcasted_iota(jnp.int32, (n, n), 1)).astype(jnp.float32)
    inverse = eliminate(0.5 * (gram[...] + gram[...].T), eye)
    p, q = flat(prev, range(s), s), flat(prev_img, range(s), s)
    gram_pq = dot_nt(p, q)

    wait(land, recv_sem.at[0])
    wait(halo, recv_sem.at[1])
    rows = jnp.concatenate([halo[i] for i in range(n)], axis=0)
    outside = jnp.where(gy == 0, 0, s - 1)

    def extended(i):
        shift = lax.rem((2 * s - i + outside) * depth, width)
        beside = jnp.where(lanes // depth == outside, pltpu.roll(rows, shift, 1), 0.0)
        return jnp.concatenate([land[pl.ds(i, n, stride=s), :], beside], axis=1)

    def give(first, count, arrived):
        target = back.at[pl.ds(column * stretch + first, count), :]
        for near, oc, where in flock:
            if near:
                remote(done.at[pl.ds(oc * stretch + first, count), :], target, 1, arrived, where)
        pltpu.make_async_copy(
            done.at[pl.ds(column * stretch + first, count), :], target, recv_sem.at[arrived]
        ).start()

    def emit(step, forward, state):
        if step not in (1, 3, 4, 6):
            return
        final = 0 if step < 4 else 1
        odd = 1 if step in (3, 4) else 0
        values = state if final else forward
        for x, z in planes:
            if x % 2 == odd:
                done[pl.ds(place_of(x, z, final), n, stride=stretch), :] = values[x, z][:, :width]
        give(place_of(odd, 0, final), half, 2 + final)

    field = [[extended(x * lz + z) for z in range(lz)] for x in range(lx)]
    image = smooth(field, ngx, ngz, gy, width, emit)
    for i, (x, z) in enumerate(planes):
        done[pl.ds(4 * s + i, n, stride=stretch), :] = image[x, z][:, :width]
    give(4 * s, s, 4)

    def share(index, sums):
        part[index] = pack(sums)
        for _, _, where in flock:
            remote(part.at[index], parts.at[index, place], 2 + index, 5 + index, where)
        pltpu.make_async_copy(part.at[index], parts.at[index, place], recv_sem.at[5 + index]).start()

    def shared(index):
        wait(parts.at[index], recv_sem.at[5 + index])
        total = unpack(tree_sum([parts[index, i] for i in range(everyone)]), 2 * n)
        return total[:, :n], total[:, n:]

    wait(back.at[pl.ds(0, n * s), :], recv_sem.at[2])
    yf = flat(back, [place_of(x, z, 0) for x, z in planes], stretch)
    share(0, jnp.concatenate([26.0 * dot_nt(yf, yf), gram_pq], axis=1))

    wait(back.at[pl.ds(0, n * s), :], recv_sem.at[3])
    zf = flat(back, [place_of(x, z, 1) for x, z in planes], stretch)
    uf = zf - yf
    share(1, jnp.concatenate([dot_nt(uf, uf), dot_nt(zf, q)], axis=1))

    gram_zr, gram_pq = shared(0)
    beta = dot(inverse, gram_zr)
    beta_t = beta.T
    known = gram_zr + dot(beta_t, dot(gram_pq, beta))
    mixed = dot(beta_t, jnp.concatenate([p, q], axis=1))
    direction = zf + mixed[:, : s * width]
    wait(back.at[pl.ds(0, n * s), :], recv_sem.at[4])
    wf = flat(back, [4 * s + i for i in range(s)], stretch)
    both = jnp.concatenate([direction, wf + mixed[:, s * width :]], axis=1)
    for i in range(s):
        dir_out[pl.ds(i, n, stride=s), :] = direction[:, i * width : (i + 1) * width]
    loads[4].wait()
    wait(done.at[pl.ds(0, (n - 1) * s + n), :], send_sem.at[0])
    wait(done.at[pl.ds(0, (n - 1) * 3 * s), :], send_sem.at[1])
    wait(parts.at[0, pl.ds(0, everyone - 1)], send_sem.at[2])

    gram_uu, gram_zq = shared(1)
    curvature = known - 26.0 * gram_uu + dot(gram_zq, beta) + dot_nt(beta_t, gram_zq)
    alpha = eliminate(curvature, gram_zr)
    step = dot(alpha.T, both)
    for i in range(s):
        rows = pl.ds(i, n, stride=s)
        sol_out[rows, :] = sol[rows, :] + step[:, i * width : (i + 1) * width]
        res_out[rows, :] = res[rows, :] - step[:, (s + i) * width : (s + i + 1) * width]
    wait(parts.at[1, pl.ds(0, everyone - 1)], send_sem.at[3])


def write(*refs):
    half = len(refs) // 2
    semaphore = refs[-1]
    stores = [pltpu.make_async_copy(refs[i], refs[half + i], semaphore.at[i]) for i in range(half)]
    for store in stores:
        store.start()
    for store in stores:
        store.wait()


def whole_body(sizes, *args):
    ngx, ngy, ngz, n, lx, lz, width = sizes
    s, everyone = lx * lz, n * ngy
    rows = n * s
    shape = args[0].shape
    field = jax.ShapeDtypeStruct((rows, width), jnp.float32)
    anywhere = pl.BlockSpec(memory_space=pl.ANY)
    inside = pl.BlockSpec(memory_space=pltpu.VMEM)
    block = pltpu.VMEM((rows, width), jnp.float32)
    packed = 2 * n * n // 128
    outs = pl.pallas_call(
        functools.partial(kernel, sizes),
        out_shape=(block,) * 3,
        in_specs=[anywhere] * 5,
        out_specs=[inside] * 3,
        scratch_shapes=[
            block, block, block, block,
            pltpu.VMEM((n, n), jnp.float32),
            block,
            pltpu.VMEM((n, 1, width), jnp.float32),
            pltpu.VMEM((n, 1, width), jnp.float32),
            pltpu.VMEM((5 * rows, width), jnp.float32),
            pltpu.VMEM((5 * rows, width), jnp.float32),
            pltpu.VMEM((2, packed, 128), jnp.float32),
            pltpu.VMEM((2, everyone, packed, 128), jnp.float32),
            pltpu.SemaphoreType.DMA((5,)),
            pltpu.SemaphoreType.DMA((4,)),
            pltpu.SemaphoreType.DMA((7,)),
        ],
        compiler_params=pltpu.CompilerParams(
            collective_id=0, has_side_effects=True
        ),
    )(*(a.reshape(rows, width) for a in args[:4]), args[4])
    outs = [pltpu.with_memory_space_constraint(a, pltpu.VMEM) for a in outs]
    outs = pl.pallas_call(
        write,
        out_shape=(field,) * 3,
        in_specs=[inside] * 3,
        out_specs=[anywhere] * 3,
        scratch_shapes=[pltpu.SemaphoreType.DMA((3,))],

    )(*outs)
    return tuple(a.reshape(shape) for a in outs)


def pick_body(mesh, solution, residual, direction_prev, image_prev, gram_prev):
    ngx, ngy, ngz = (mesh.shape[axis] for axis in ("gx", "gy", "gz"))
    n, lx, lz, width = residual.shape
    fits = n == ngx * ngz and lx % 2 == 0 and lz % 2 == 0 and (lx * lz) % 8 == 0
    fits = fits and width % 128 == 0 and n % 16 == 0 and 128 % (2 * n) == 0 and ngy == 2 and width % (lx * lz) == 0 and width // (lx * lz) >= 15
    args = (solution, residual, direction_prev, image_prev, gram_prev)
    if fits:
        return whole_body((ngx, ngy, ngz, n, lx, lz, width), *args)
    return body(*args)


def solution(mesh):
    in_specs = (
        P(None, "gx", "gz", "gy"),
        P(None, "gx", "gz", "gy"),
        P(None, "gx", "gz", "gy"),
        P(None, "gx", "gz", "gy"),
        P(),
    )
    out_specs = (P(None, "gx", "gz", "gy"), P(None, "gx", "gz", "gy"), P(None, "gx", "gz", "gy"))
    return jax.shard_map(functools.partial(pick_body, mesh), mesh=mesh, in_specs=in_specs, out_specs=out_specs, check_vma=False)
```

```python
import functools

import jax
import jax.numpy as jnp
from jax import lax
from jax.experimental import pallas as pl
from jax.experimental.pallas import tpu as pltpu
from jax.sharding import PartitionSpec as P


def with_halo(value, sides, width):
    for axis, dim in sides:
        devices, length = (lax.axis_size(axis), value.shape[dim])
        up = [(i, (i + 1) % devices) for i in range(devices - 1)]
        down = [(j, i) for i, j in up]
        last = lax.slice_in_dim(value, length - width, length, axis=dim)
        first = lax.slice_in_dim(value, 0, width, axis=dim)
        before = lax.ppermute(last, axis, up)
        after = lax.ppermute(first, axis, down)
        value = jnp.concatenate([before, value, after], axis=dim)
    return value


def box_sum(padded):
    total = padded[:, :-2] + padded[:, 1:-1] + padded[:, 2:]
    total = total[:, :, :-2] + total[:, :, 1:-1] + total[:, :, 2:]
    return total[:, :, :, :-2] + total[:, :, :, 1:-1] + total[:, :, :, 2:]


def colors_of(shape):
    first = lax.broadcasted_iota(jnp.int32, shape, 1) % 2
    second = lax.broadcasted_iota(jnp.int32, shape, 2) % 2
    third = lax.broadcasted_iota(jnp.int32, shape, 3) % 2
    return 4 * first + 2 * second + third


def local_gram(left, right):
    return jnp.einsum("kxzy,lxzy->kl", left, right, precision=lax.Precision.HIGHEST)


def combine(field, mixing):
    return jnp.einsum("kxzy,kl->lxzy", field, mixing, precision=lax.Precision.HIGHEST)


def small_dot(left, right):
    return jnp.dot(left, right, precision=lax.Precision.HIGHEST)


def spd_solve(matrix, target):
    order = matrix.shape[0]
    sym = 0.5 * (matrix + matrix.T)
    lower = jnp.zeros_like(sym)
    for col in range(order):
        column = sym[col:, col] - jnp.sum(lower[col:, :col] * lower[col, :col][None, :], axis=1)
        pivot = jnp.sqrt(column[0])
        lower = lower.at[col:, col].set(column / pivot)
    middle = jnp.zeros_like(target)
    for row in range(order):
        value = target[row] - jnp.sum(lower[row, :row][:, None] * middle[:row], axis=0)
        middle = middle.at[row].set(value / lower[row, row])
    answer = jnp.zeros_like(target)
    for row in range(order - 1, -1, -1):
        value = middle[row] - jnp.sum(lower[row + 1 :, row][:, None] * answer[row + 1 :], axis=0)
        answer = answer.at[row].set(value / lower[row, row])
    return answer


def sweep_box(field):
    padded = with_halo(field, (("gx", 1), ("gy", 3), ("gz", 2)), 1)
    return box_sum(padded)


def body(solution, residual, direction_prev, image_prev, gram_prev):
    colors = colors_of(residual.shape)
    smoothed = jnp.where(colors == 0, residual / 26.0, jnp.float32(0.0))
    for shade in list(range(1, 8)) + list(range(6, -1, -1)):
        boxed = sweep_box(smoothed)
        smoothed = jnp.where(colors == shade, (residual + boxed - smoothed) / 26.0, smoothed)
    padded = with_halo(smoothed, (("gx", 1), ("gy", 3), ("gz", 2)), 1)
    image = 27.0 * smoothed - box_sum(padded)
    sums = (
        local_gram(smoothed, residual),
        local_gram(smoothed, image),
        local_gram(smoothed, image_prev),
        local_gram(direction_prev, image),
        local_gram(direction_prev, image_prev),
    )
    gram_zr, gram_zw, gram_zq, gram_pw, gram_pq = lax.psum(
        (sums[0], sums[1], sums[2], sums[3], sums[4]), ("gx", "gy", "gz")
    )
    beta_mix = spd_solve(gram_prev, gram_zr)
    direction = smoothed + combine(direction_prev, beta_mix)
    image_new = image + combine(image_prev, beta_mix)
    curvature = gram_zw + small_dot(gram_zq, beta_mix) + small_dot(beta_mix.T, gram_pw)
    curvature = curvature + small_dot(small_dot(beta_mix.T, gram_pq), beta_mix)
    alpha_step = spd_solve(curvature, gram_zr)
    solution_new = solution + combine(direction, alpha_step)
    residual_new = residual - combine(image_new, alpha_step)
    return (solution_new, residual_new, direction)


MESH = pl.DeviceIdType.MESH
HIGHEST = lax.Precision.HIGHEST


def dot(left, right):
    return jnp.dot(left, right, precision=HIGHEST, preferred_element_type=jnp.float32)


def dot_nt(left, right):
    return lax.dot_general(
        left, right, (((1,), (1,)), ((), ())), precision=HIGHEST, preferred_element_type=jnp.float32
    )


def eliminate(matrix, target):
    order = matrix.shape[0]
    rows = lax.broadcasted_iota(jnp.int32, matrix.shape, 0)
    columns = [jnp.broadcast_to(matrix[:, k : k + 1], matrix.shape) for k in range(order)]
    scale = jnp.zeros(matrix.shape, jnp.float32)
    for c in range(order):
        inverse = 1.0 / columns[c][c : c + 1, :]
        here = rows == c
        factor = jnp.where(here, 0.0, columns[c] * inverse)
        for k in range(c + 1, order):
            columns[k] = columns[k] - factor * columns[k][c : c + 1, :]
        target = target - factor * target[c : c + 1, :]
        scale = jnp.where(here, inverse, scale)
    return target * scale


def smooth(res, ngx, ngz, gy, whole, emit):
    lx, lz = len(res), len(res[0])
    count, ny = res[0][0].shape
    row = lax.broadcasted_iota(jnp.int32, (count, ny), 0)
    lane = lax.broadcasted_iota(jnp.int32, (count, ny), 1)
    even = lane % 2 == 0
    inner = row % (ngx * ngz)
    edges = {
        "xp": (inner < ngz, ngz),
        "xn": (inner >= (ngx - 1) * ngz, count - ngz),
        "zp": (row % ngz == 0, 1),
        "zn": (row % ngz == ngz - 1, count - 1),
    }
    first = jnp.where(jnp.logical_and(row < whole, gy == 0), 0, -8)
    last = jnp.where(jnp.logical_and(row < whole, gy != 0), ny - 1, -8)
    cut = jnp.where(row < whole, jnp.where(gy == 0, ny - 3, 0), -8)
    valid = jnp.logical_or(lane < cut, lane > cut + 2)
    valid_even, valid_odd = jnp.logical_and(valid, even), jnp.logical_and(valid, jnp.logical_not(even))
    twice = 2.0 - jnp.where(lane == first, 1.0, 0.0) - jnp.where(lane == last, 1.0, 0.0)
    below = 3.0 - jnp.where(lane == first + 1, 1.0, 0.0) - jnp.where(lane == last, 1.0, 0.0)
    above = 3.0 - jnp.where(lane == last - 1, 1.0, 0.0) - jnp.where(lane == first, 1.0, 0.0)
    zero = jnp.zeros((count, ny), jnp.float32)
    memo = {}

    def moved(value, kind):
        if value is None:
            return None
        key = (kind, id(value))
        if key not in memo:
            edge, amount = edges[kind]
            memo[key] = (value, jnp.where(edge, zero, pltpu.roll(value, amount, 0)))
        return memo[key][1]

    def add(*values):
        total = None
        for value in values:
            if value is not None:
                total = value if total is None else total + value
        return total

    state = {(x, z): None for x in range(lx) for z in range(lz)}

    def z_pair(x, z):
        before = state[x, z - 1] if z > 0 else moved(state[x, lz - 1], "zp")
        after = state[x, z + 1] if z < lz - 1 else moved(state[x, 0], "zn")
        return add(before, after)

    def neighbours(x, z):
        def line(other):
            return add(state[other, z], z_pair(other, z))

        before = line(x - 1) if x > 0 else moved_line(lx - 1, z, "xp")
        after = line(x + 1) if x < lx - 1 else moved_line(0, z, "xn")
        return add(z_pair(x, z), before, after)

    def moved_line(x, z, kind):
        return moved(add(state[x, z], z_pair(x, z)), kind)

    def woven(at_even, at_odd):
        return jnp.where(valid_even, at_even, jnp.where(valid_odd, at_odd, zero))

    def shifted(value, k):
        return pltpu.roll(value, k, 1), pltpu.roll(value, ny - k, 1)

    def once(value):
        return sum(shifted(value, 1))

    def two(value):
        return sum(shifted(value, 2)) + twice * value

    third = jnp.float32(1.0 / 26.0)
    plan = [(0, 0), (0, 1), (1, 0), (1, 1), (1, 0), (0, 1), (0, 0)]
    forward = {}
    for step, (xp, zp) in enumerate(plan):
        fresh = {}
        for x in range(xp, lx, 2):
            for z in range(zp, lz, 2):
                near, value = neighbours(x, z), state[x, z]
                own = res[x][z]
                both = own if near is None else own + near
                share = third * both
                if value is None and near is None:
                    fresh[x, z] = jnp.where(even, share, third * (own + once(woven(share, zero))))
                    forward[x, z] = fresh[x, z]
                elif value is None:
                    mix = woven(near + share, near)
                    down, up = shifted(mix, 1)
                    pair, far = down + up, two(mix)
                    base = both + pair
                    later = third * (base + third * far)
                    fresh[x, z] = forward[x, z] = jnp.where(even, third * base, later)
                    if step == 3:
                        deep = sum(shifted(mix, 3)) + below * down + above * up
                        again = base + third * (once(woven(zero, both)) + far + third * deep)
                        fresh[x, z] = jnp.where(even, third * again, later)
                else:
                    mix = woven(near + value, near + share)
                    base = both + once(mix)
                    fresh[x, z] = third * jnp.where(even, base + third * two(mix), base)
        state.update(fresh)
        emit(step, forward, state)
    image = {}
    for x in range(lx):
        for z in range(lz):
            box = add(state[x, z], neighbours(x, z))
            image[x, z] = 27.0 * state[x, z] - (box + once(jnp.where(valid, box, zero)))
    return image


def pack(value):
    rows = value.shape[0] * value.shape[1] // 128
    return jnp.concatenate([value[i : i + rows] for i in range(0, value.shape[0], rows)], axis=1)


def unpack(value, lanes):
    return jnp.concatenate([value[:, i : i + lanes] for i in range(0, value.shape[1], lanes)], axis=0)


def tree_sum(values):
    while len(values) > 1:
        values = [sum(values[i + 1 : i + 2], values[i]) for i in range(0, len(values), 2)]
    return values[0]


def spans_of(ngz, lx, lz):
    level, spans = ngz // 2, []
    for plane in range(ngz):
        rows = []
        for x in range(lx):
            for z in range(lz):
                below = level * lz - 1 - (plane * lz + z)
                away, reach = (below, 5) if below >= 0 else (-1 - below, 6)
                if away <= reach - 2 * (x % 2):
                    rows.append(x * lz + z)
        spans.append((rows[0], rows[-1] + 1) if rows else (0, 0))
    return spans


def kernel(
    sizes, sol_in, res_in, dir_in, img_in, gram_in, sol_out, res_out, dir_out,
    sol, res, prev, prev_img, gram, land, strip, halo, done, back, part, parts, early, earlies,
    local_sem, send_sem, recv_sem,
):
    ngx, ngy, ngz, n, lx, lz, width = sizes
    s, level = lx * lz, ngz // 2
    per = n // (ngx * level)
    some = per * s
    gx, gy, gz = lax.axis_index("gx"), lax.axis_index("gy"), lax.axis_index("gz")
    column = gx * ngz + gz
    place = gy * n + column
    everyone = n * ngy

    loads = [
        pltpu.make_async_copy(a, b, local_sem.at[i])
        for i, (a, b) in enumerate(
            ((res_in, res), (gram_in, gram), (dir_in, prev), (img_in, prev_img), (sol_in, sol))
        )
    ]
    for load in loads:
        load.start()

    low = gz < level
    floors = [
        jnp.where(
            low,
            jnp.where(ngz - 1 - k > gz, ngz - 1 - k, ngz - 2 - k),
            jnp.where(k < gz, k, k + 1),
        )
        for k in range(ngz - 1)
    ] + [gz]
    across = [jnp.bitwise_xor(gx, dx) for dx in range(ngx)]
    ways = sorted(
        ((dx, dy, k) for dx in range(ngx) for dy in range(ngy) for k in range(ngz)),
        key=lambda way: (way[2] >= level, way[2] - (way[0] > 1) - way[1], -way[1], -way[0]),
    )
    flock = []
    for dx, dy, k in ways:
        if (dx, dy, k) != (0, 0, ngz - 1):
            ox, oy, oz = across[dx], 1 - gy if dy else gy, floors[k]
            owner = ox * level + jnp.bitwise_and(oz, level - 1)
            flock.append((dy == 0, k >= level, owner, ox * ngz + oz, {"gx": ox, "gy": oy, "gz": oz}))
    owner = gx * level + jnp.bitwise_and(gz, level - 1)

    def remote(source, target, sent, arrived, where):
        pltpu.make_async_remote_copy(
            src_ref=source, dst_ref=target, send_sem=send_sem.at[sent], recv_sem=recv_sem.at[arrived],
            device_id=where, device_id_type=MESH,
        ).start()

    def wait(ref, semaphore):
        pltpu.make_async_copy(ref, ref, semaphore).wait()

    land[...] = jnp.zeros_like(land)
    barrier = pltpu.get_barrier_semaphore()
    for peer in flock:
        pl.semaphore_signal(barrier, inc=1, device_id=peer[4], device_id_type=MESH)
    loads[0].wait()
    depth = width // s
    lanes = lax.broadcasted_iota(jnp.int32, (n, width), 1)
    packed = jnp.zeros((n, width), jnp.float32)
    for i in range(s):
        line = res[pl.ds(i, n, stride=s), :]
        line = pltpu.roll(line, lax.rem(i * depth + jnp.where(gy == 0, depth, 0), width), 1)
        packed = jnp.where(lanes // depth == i, line, packed)
    for i in range(n):
        strip[i] = packed[i : i + 1, :]
    pl.semaphore_wait(barrier, everyone - 1)

    mine = land.at[pl.ds(column * some, some), :]
    spans = spans_of(ngz, lx, lz)

    def by_plane(work):
        for span in sorted(set(spans)):
            here = functools.reduce(jnp.logical_or, [gz == g for g in range(ngz) if spans[g] == span])
            pl.when(here)(functools.partial(work, *span))

    def cross(begin, end):
        for same, level_with, into, _, where in flock:
            if same and not level_with:
                remote(
                    res.reshape(n, s, width).at[pl.ds(into * per, per), pl.ds(begin, end - begin), :],
                    land.reshape(per * n, s, width).at[pl.ds(column * per, per), pl.ds(begin, end - begin), :],
                    6, 8, where,
                )

    def edges(level_with_me):
        for same, level_with, into, _, where in flock:
            if not same and level_with == level_with_me:
                remote(strip.at[pl.ds(into * per, per)], halo.at[pl.ds(column * per, per)], 5, 1, where)

    edges(False)
    by_plane(cross)
    edges(True)
    for same, level_with, into, _, where in flock:
        if same and level_with:
            remote(res.at[pl.ds(into * some, some), :], mine, 0, 0, where)
    pltpu.make_async_copy(res.at[pl.ds(owner * some, some), :], mine, recv_sem.at[0]).start()

    def flat(ref, first, stride):
        return jnp.concatenate([ref[pl.ds(first + i, n, stride=stride), :] for i in range(s)], axis=1)

    def send_all(source, target, sent, arrived):
        for peer in flock:
            remote(source, target, sent, arrived, peer[4])
        pltpu.make_async_copy(source, target, recv_sem.at[arrived]).start()

    planes = [(x, z) for x in range(lx) for z in range(lz)]
    for load in loads[1:4]:
        load.wait()
    p, q = flat(prev, 0, s), flat(prev_img, 0, s)
    early[0] = pack(dot_nt(p, q))
    eye = (lax.broadcasted_iota(jnp.int32, (n, n), 0) == lax.broadcasted_iota(jnp.int32, (n, n), 1)).astype(jnp.float32)
    inverse = eliminate(0.5 * (gram[...] + gram[...].T), eye)

    wait(land.at[pl.ds(0, level * ngx * some), :], recv_sem.at[0])
    above = ngx * per * sum(end - begin for begin, end in spans[level:])
    below = ngx * per * sum(end - begin for begin, end in spans[:level])

    @pl.when(low)
    def _():
        wait(land.at[pl.ds(0, above), :], recv_sem.at[8])

    @pl.when(jnp.logical_not(low))
    def _():
        wait(land.at[pl.ds(0, below), :], recv_sem.at[8])

    wait(halo, recv_sem.at[1])
    beyond = [jnp.concatenate([halo[i * per + a] for i in range(n)], axis=0) for a in range(per)]
    zone = width // per
    outer = jnp.where(gy == 0, zone - depth, 0)
    shift = jnp.where(gy == 0, zone, depth)

    def extended(i):
        lines = [land[pl.ds(a * s + i, n, stride=some), :] for a in range(per)]
        edge = None
        for a in range(per):
            begin = a * zone
            inside = pltpu.roll(lines[a], lax.rem(begin + shift + jnp.where(gy == 0, width - depth, 0), width), 1)
            outside = pltpu.roll(beyond[a], lax.rem(begin + outer + width - i * depth, width), 1)
            at = lanes - (begin + outer)
            value = jnp.where(jnp.logical_and(at >= 0, at < depth), outside, inside)
            edge = value if edge is None else jnp.where(lanes >= begin, value, edge)
        return jnp.concatenate(lines + [edge], axis=0)

    border = jnp.where(gy == 0, width - depth, 0)
    at_border = jnp.logical_and(lanes >= border, lanes < border + depth)

    def keep(field, values):
        for i, (x, z) in enumerate(planes):
            edge = values[x, z][per * n :]
            for a in range(per):
                back_shift = lax.rem(2 * width - a * zone - shift - jnp.where(gy == 0, width - depth, 0), width)
                value = jnp.where(at_border, pltpu.roll(edge, back_shift, 1), values[x, z][a * n : (a + 1) * n])
                done[field, pl.ds(a * s + i, n, stride=some), :] = value
        target = back.at[field, pl.ds(owner * some, some), :]
        for same, level_with, _, home, where in flock:
            if same and level_with:
                remote(done.at[field, pl.ds(home * some, some), :], target, 1, 2 + field, where)
        pltpu.make_async_copy(done.at[field, pl.ds(column * some, some), :], target, recv_sem.at[2 + field]).start()

    def emit(step, forward, state):
        if step == 3:
            keep(0, forward)
        if step == 6:
            keep(1, state)

    field = [[extended(x * lz + z) for z in range(lz)] for x in range(lx)]
    keep(2, smooth(field, ngx, ngz, gy, per * n, emit))
    send_all(early.at[0], earlies.at[0, place], 2, 5)

    wait(back.at[0], recv_sem.at[2])
    yf = flat(back.at[0], 0, s)
    early[1] = pack(26.0 * dot_nt(yf, yf))
    send_all(early.at[1], earlies.at[1, place], 3, 6)

    wait(back.at[1], recv_sem.at[3])
    zf = flat(back.at[1], 0, s)
    uf = zf - yf
    part[...] = pack(jnp.concatenate([dot_nt(uf, uf), dot_nt(zf, q)], axis=1))
    send_all(part, parts.at[place], 4, 7)

    def summed(ref):
        return tree_sum([ref[i] for i in range(everyone)])

    wait(earlies.at[0], recv_sem.at[5])
    gram_pq = unpack(summed(earlies.at[0]), n)
    wait(earlies.at[1], recv_sem.at[6])
    gram_zr = unpack(summed(earlies.at[1]), n)
    beta = dot(inverse, gram_zr)
    beta_t = beta.T
    known = gram_zr + dot(beta_t, dot(gram_pq, beta))
    mixed = dot(beta_t, jnp.concatenate([p, q], axis=1))
    direction = zf + mixed[:, : s * width]
    wait(back.at[2], recv_sem.at[4])
    wf = flat(back.at[2], 0, s)
    both = jnp.concatenate([direction, wf + mixed[:, s * width :]], axis=1)
    for i in range(s):
        dir_out[pl.ds(i, n, stride=s), :] = direction[:, i * width : (i + 1) * width]
    loads[4].wait()
    wait(land.at[pl.ds(0, (level * ngx - 1) * some), :], send_sem.at[0])
    by_plane(lambda begin, end: wait(land.at[pl.ds(0, level * ngx * per * (end - begin)), :], send_sem.at[6]))
    wait(halo, send_sem.at[5])
    wait(back.at[pl.ds(0, 3), pl.ds(0, (n // per - 1) * some), :], send_sem.at[1])
    wait(earlies.at[0, pl.ds(0, everyone - 1)], send_sem.at[2])
    wait(earlies.at[1, pl.ds(0, everyone - 1)], send_sem.at[3])

    wait(parts, recv_sem.at[7])
    total = unpack(summed(parts), 2 * n)
    gram_uu, gram_zq = total[:, :n], total[:, n:]
    curvature = known - 26.0 * gram_uu + dot(gram_zq, beta) + dot_nt(beta_t, gram_zq)
    alpha = eliminate(curvature, gram_zr)
    step = dot(alpha.T, both)
    for i in range(s):
        rows = pl.ds(i, n, stride=s)
        sol_out[rows, :] = sol[rows, :] + step[:, i * width : (i + 1) * width]
        res_out[rows, :] = res[rows, :] - step[:, (s + i) * width : (s + i + 1) * width]
    wait(parts.at[pl.ds(0, everyone - 1)], send_sem.at[4])


def write(*refs):
    half = len(refs) // 2
    semaphore = refs[-1]
    stores = [pltpu.make_async_copy(refs[i], refs[half + i], semaphore.at[i]) for i in range(half)]
    for store in stores:
        store.start()
    for store in stores:
        store.wait()


def whole_body(sizes, *args):
    ngx, ngy, ngz, n, lx, lz, width = sizes
    s, everyone = lx * lz, n * ngy
    rows = n * s
    shape = args[0].shape
    field = jax.ShapeDtypeStruct((rows, width), jnp.float32)
    anywhere = pl.BlockSpec(memory_space=pl.ANY)
    inside = pl.BlockSpec(memory_space=pltpu.VMEM)
    block = pltpu.VMEM((rows, width), jnp.float32)
    per = 2 * n // (ngx * ngz)
    packed = n * n // 128
    outs = pl.pallas_call(
        functools.partial(kernel, sizes),
        out_shape=(block,) * 3,
        in_specs=[anywhere] * 5,
        out_specs=[inside] * 3,
        scratch_shapes=[
            block, block, block, block,
            pltpu.VMEM((n, n), jnp.float32),
            pltpu.VMEM((per * rows, width), jnp.float32),
            pltpu.VMEM((n, 1, width), jnp.float32),
            pltpu.VMEM((per * n, 1, width), jnp.float32),
            pltpu.VMEM((3, per * rows, width), jnp.float32),
            pltpu.VMEM((3, rows, width), jnp.float32),
            pltpu.VMEM((2 * packed, 128), jnp.float32),
            pltpu.VMEM((everyone, 2 * packed, 128), jnp.float32),
            pltpu.VMEM((2, packed, 128), jnp.float32),
            pltpu.VMEM((2, everyone, packed, 128), jnp.float32),
            pltpu.SemaphoreType.DMA((5,)),
            pltpu.SemaphoreType.DMA((7,)),
            pltpu.SemaphoreType.DMA((9,)),
        ],
        compiler_params=pltpu.CompilerParams(
            collective_id=0, has_side_effects=True
        ),
    )(*(a.reshape(rows, width) for a in args[:4]), args[4])
    outs = [pltpu.with_memory_space_constraint(a, pltpu.VMEM) for a in outs]
    outs = pl.pallas_call(
        write,
        out_shape=(field,) * 3,
        in_specs=[inside] * 3,
        out_specs=[anywhere] * 3,
        scratch_shapes=[pltpu.SemaphoreType.DMA((3,))],

    )(*outs)
    return tuple(a.reshape(shape) for a in outs)


def pick_body(mesh, solution, residual, direction_prev, image_prev, gram_prev):
    ngx, ngy, ngz = (mesh.shape[axis] for axis in ("gx", "gy", "gz"))
    n, lx, lz, width = residual.shape
    fits = n == ngx * ngz and lx % 2 == 0 and lz % 2 == 0 and (lx * lz) % 8 == 0
    fits = fits and width % 128 == 0 and n % 16 == 0 and 128 % (2 * n) == 0 and ngy == 2 and ngz > 1 and width >= 4 * (width // (lx * lz)) and (ngx & (ngx - 1)) == 0 and (ngz & (ngz - 1)) == 0 and width % (lx * lz) == 0 and width // (lx * lz) >= 15
    args = (solution, residual, direction_prev, image_prev, gram_prev)
    if fits:
        return whole_body((ngx, ngy, ngz, n, lx, lz, width), *args)
    return body(*args)


def solution(mesh):
    in_specs = (
        P(None, "gx", "gz", "gy"),
        P(None, "gx", "gz", "gy"),
        P(None, "gx", "gz", "gy"),
        P(None, "gx", "gz", "gy"),
        P(),
    )
    out_specs = (P(None, "gx", "gz", "gy"), P(None, "gx", "gz", "gy"), P(None, "gx", "gz", "gy"))
    return jax.shard_map(functools.partial(pick_body, mesh), mesh=mesh, in_specs=in_specs, out_specs=out_specs, check_vma=False)
```

```python
import functools

import jax
import jax.numpy as jnp
from jax import lax
from jax.experimental import pallas as pl
from jax.experimental.pallas import tpu as pltpu
from jax.sharding import PartitionSpec as P


def with_halo(value, sides, width):
    for axis, dim in sides:
        devices, length = (lax.axis_size(axis), value.shape[dim])
        up = [(i, (i + 1) % devices) for i in range(devices - 1)]
        down = [(j, i) for i, j in up]
        last = lax.slice_in_dim(value, length - width, length, axis=dim)
        first = lax.slice_in_dim(value, 0, width, axis=dim)
        before = lax.ppermute(last, axis, up)
        after = lax.ppermute(first, axis, down)
        value = jnp.concatenate([before, value, after], axis=dim)
    return value


def box_sum(padded):
    total = padded[:, :-2] + padded[:, 1:-1] + padded[:, 2:]
    total = total[:, :, :-2] + total[:, :, 1:-1] + total[:, :, 2:]
    return total[:, :, :, :-2] + total[:, :, :, 1:-1] + total[:, :, :, 2:]


def colors_of(shape):
    first = lax.broadcasted_iota(jnp.int32, shape, 1) % 2
    second = lax.broadcasted_iota(jnp.int32, shape, 2) % 2
    third = lax.broadcasted_iota(jnp.int32, shape, 3) % 2
    return 4 * first + 2 * second + third


def local_gram(left, right):
    return jnp.einsum("kxzy,lxzy->kl", left, right, precision=lax.Precision.HIGHEST)


def combine(field, mixing):
    return jnp.einsum("kxzy,kl->lxzy", field, mixing, precision=lax.Precision.HIGHEST)


def small_dot(left, right):
    return jnp.dot(left, right, precision=lax.Precision.HIGHEST)


def spd_solve(matrix, target):
    order = matrix.shape[0]
    sym = 0.5 * (matrix + matrix.T)
    lower = jnp.zeros_like(sym)
    for col in range(order):
        column = sym[col:, col] - jnp.sum(lower[col:, :col] * lower[col, :col][None, :], axis=1)
        pivot = jnp.sqrt(column[0])
        lower = lower.at[col:, col].set(column / pivot)
    middle = jnp.zeros_like(target)
    for row in range(order):
        value = target[row] - jnp.sum(lower[row, :row][:, None] * middle[:row], axis=0)
        middle = middle.at[row].set(value / lower[row, row])
    answer = jnp.zeros_like(target)
    for row in range(order - 1, -1, -1):
        value = middle[row] - jnp.sum(lower[row + 1 :, row][:, None] * answer[row + 1 :], axis=0)
        answer = answer.at[row].set(value / lower[row, row])
    return answer


def sweep_box(field):
    padded = with_halo(field, (("gx", 1), ("gy", 3), ("gz", 2)), 1)
    return box_sum(padded)


def body(solution, residual, direction_prev, image_prev, gram_prev):
    colors = colors_of(residual.shape)
    smoothed = jnp.where(colors == 0, residual / 26.0, jnp.float32(0.0))
    for shade in list(range(1, 8)) + list(range(6, -1, -1)):
        boxed = sweep_box(smoothed)
        smoothed = jnp.where(colors == shade, (residual + boxed - smoothed) / 26.0, smoothed)
    padded = with_halo(smoothed, (("gx", 1), ("gy", 3), ("gz", 2)), 1)
    image = 27.0 * smoothed - box_sum(padded)
    sums = (
        local_gram(smoothed, residual),
        local_gram(smoothed, image),
        local_gram(smoothed, image_prev),
        local_gram(direction_prev, image),
        local_gram(direction_prev, image_prev),
    )
    gram_zr, gram_zw, gram_zq, gram_pw, gram_pq = lax.psum(
        (sums[0], sums[1], sums[2], sums[3], sums[4]), ("gx", "gy", "gz")
    )
    beta_mix = spd_solve(gram_prev, gram_zr)
    direction = smoothed + combine(direction_prev, beta_mix)
    image_new = image + combine(image_prev, beta_mix)
    curvature = gram_zw + small_dot(gram_zq, beta_mix) + small_dot(beta_mix.T, gram_pw)
    curvature = curvature + small_dot(small_dot(beta_mix.T, gram_pq), beta_mix)
    alpha_step = spd_solve(curvature, gram_zr)
    solution_new = solution + combine(direction, alpha_step)
    residual_new = residual - combine(image_new, alpha_step)
    return (solution_new, residual_new, direction)


MESH = pl.DeviceIdType.MESH
HIGHEST = lax.Precision.HIGHEST


def dot(left, right):
    return jnp.dot(left, right, precision=HIGHEST, preferred_element_type=jnp.float32)


def dot_nt(left, right):
    return lax.dot_general(
        left, right, (((1,), (1,)), ((), ())), precision=HIGHEST, preferred_element_type=jnp.float32
    )


def parts_of(value):
    first = value.astype(jnp.bfloat16)
    rest = value - first.astype(jnp.float32)
    second = rest.astype(jnp.bfloat16)
    third = (rest - second.astype(jnp.float32)).astype(jnp.bfloat16)
    return first, second, third


def product(left, right, contract):
    order = left[0].shape[0]
    total = None
    for i, term in enumerate(right):
        stack = jnp.concatenate(left[: 3 - i], axis=0) if i < 2 else left[0]
        out = lax.dot_general(stack, term, (contract, ((), ())), preferred_element_type=jnp.float32)
        for j in range(3 - i):
            piece = out[j * order : (j + 1) * order]
            total = piece if total is None else total + piece
    return total


def gram_of(left, right):
    return product(left, right, ((1,), (1,)))


def small(left, right):
    return product(parts_of(left), parts_of(right), ((1,), (0,)))


def wide(turned, right):
    a, b, c = (v.astype(jnp.float32) for v in parts_of(turned))
    d, e, f = right
    left = jnp.concatenate([a, a, b, b, a, c], axis=0).T.astype(jnp.bfloat16)
    return jnp.dot(left, jnp.concatenate([d, e, d, e, f, d], axis=0), preferred_element_type=jnp.float32)


def eliminate(matrix, target):
    order = matrix.shape[0]
    rows = lax.broadcasted_iota(jnp.int32, matrix.shape, 0)
    columns = [jnp.broadcast_to(matrix[:, k : k + 1], matrix.shape) for k in range(order)]
    scale = jnp.zeros(matrix.shape, jnp.float32)
    for c in range(order):
        inverse = 1.0 / columns[c][c : c + 1, :]
        here = rows == c
        factor = jnp.where(here, 0.0, columns[c] * inverse)
        for k in range(c + 1, order):
            columns[k] = columns[k] - factor * columns[k][c : c + 1, :]
        target = target - factor * target[c : c + 1, :]
        scale = jnp.where(here, inverse, scale)
    return target * scale


def smooth(res, ngx, ngz, gy, ends):
    lx, lz = len(res), len(res[0])
    count, ny = res[0][0].shape
    row = lax.broadcasted_iota(jnp.int32, (count, ny), 0)
    lane = lax.broadcasted_iota(jnp.int32, (count, ny), 1)
    even = lane % 2 == 0
    edges = {
        "xp": (row < ngz, ngz),
        "xn": (row >= (ngx - 1) * ngz, count - ngz),
        "zp": (row % ngz == 0, 1),
        "zn": (row % ngz == ngz - 1, count - 1),
    }
    odd = jnp.logical_not(even)
    if ends:
        first, last = jnp.where(gy == 0, 0, -8), jnp.where(gy == 0, -8, ny - 1)
        cut = jnp.where(gy == 0, ny - 3, 0)
        valid = jnp.logical_or(lane < cut, lane > cut + 2)
        valid_even, valid_odd = jnp.logical_and(valid, even), jnp.logical_and(valid, odd)
        twice = 2.0 - jnp.where(jnp.logical_or(lane == first, lane == last), 1.0, 0.0)
        below = 3.0 - jnp.where(jnp.logical_or(lane == first + 1, lane == last), 1.0, 0.0)
        above = 3.0 - jnp.where(jnp.logical_or(lane == last - 1, lane == first), 1.0, 0.0)
    else:
        twice, below, above = jnp.float32(2.0), jnp.float32(3.0), jnp.float32(3.0)
    zero = jnp.zeros((count, ny), jnp.float32)
    memo = {}

    def moved(value, kind):
        if value is None:
            return None
        key = (kind, id(value))
        if key not in memo:
            edge, amount = edges[kind]
            memo[key] = (value, jnp.where(edge, zero, pltpu.roll(value, amount, 0)))
        return memo[key][1]

    def add(*values):
        total = None
        for value in values:
            if value is not None:
                total = value if total is None else total + value
        return total

    state = {(x, z): None for x in range(lx) for z in range(lz)}

    def z_pair(x, z):
        before = state[x, z - 1] if z > 0 else moved(state[x, lz - 1], "zp")
        after = state[x, z + 1] if z < lz - 1 else moved(state[x, 0], "zn")
        return add(before, after)

    def neighbours(x, z):
        def line(other):
            return add(state[other, z], z_pair(other, z))

        before = line(x - 1) if x > 0 else moved_line(lx - 1, z, "xp")
        after = line(x + 1) if x < lx - 1 else moved_line(0, z, "xn")
        return add(z_pair(x, z), before, after)

    def moved_line(x, z, kind):
        return moved(add(state[x, z], z_pair(x, z)), kind)

    def woven(at_even, at_odd):
        if not ends:
            return jnp.where(even, at_even, at_odd)
        return jnp.where(valid_even, at_even, jnp.where(valid_odd, at_odd, zero))

    def shifted(value, k):
        return pltpu.roll(value, k, 1), pltpu.roll(value, ny - k, 1)

    def once(value):
        return sum(shifted(value, 1))

    def two(value):
        return sum(shifted(value, 2)) + twice * value

    third = jnp.float32(1.0 / 26.0)
    plan = [(0, 0), (0, 1), (1, 0), (1, 1), (1, 0), (0, 1), (0, 0)]
    forward = {}
    for step, (xp, zp) in enumerate(plan):
        fresh = {}
        for x in range(xp, lx, 2):
            for z in range(zp, lz, 2):
                near, value = neighbours(x, z), state[x, z]
                own = res[x][z]
                both = own if near is None else own + near
                share = third * both
                if value is None and near is None:
                    fresh[x, z] = jnp.where(even, share, third * (own + once(woven(share, zero))))
                    forward[x, z] = fresh[x, z]
                elif value is None:
                    mix = woven(near + share, near)
                    down, up = shifted(mix, 1)
                    pair, far = down + up, two(mix)
                    base = both + pair
                    later = third * (base + third * far)
                    fresh[x, z] = forward[x, z] = jnp.where(even, third * base, later)
                    if step == 3:
                        deep = sum(shifted(mix, 3)) + below * down + above * up
                        again = base + third * (once(woven(zero, both)) + far + third * deep)
                        fresh[x, z] = jnp.where(even, third * again, later)
                else:
                    mix = woven(near + value, near + share)
                    base = both + once(mix)
                    fresh[x, z] = third * jnp.where(even, base + third * two(mix), base)
        state.update(fresh)
        yield forward, state
    image = {}
    for x in range(lx):
        for z in range(lz):
            box = add(state[x, z], neighbours(x, z))
            image[x, z] = 27.0 * state[x, z] - (box + once(jnp.where(valid, box, zero) if ends else box))
    yield image, None


def pack(value):
    rows = value.shape[0] * value.shape[1] // 128
    return jnp.concatenate([value[i : i + rows] for i in range(0, value.shape[0], rows)], axis=1)


def unpack(value, lanes):
    return jnp.concatenate([value[:, i : i + lanes] for i in range(0, value.shape[1], lanes)], axis=0)


def tree_sum(values):
    while len(values) > 1:
        values = [sum(values[i + 1 : i + 2], values[i]) for i in range(0, len(values), 2)]
    return values[0]


def spans_of(ngz, lx, lz):
    level, spans = ngz // 2, []
    for plane in range(ngz):
        rows = []
        for x in range(lx):
            for z in range(lz):
                below = level * lz - 1 - (plane * lz + z)
                away, reach = (below, 5) if below >= 0 else (-1 - below, 6)
                if away <= reach - 2 * (x % 2):
                    rows.append(x * lz + z)
        spans.append((rows[0], rows[-1] + 1) if rows else (0, 0))
    return spans


def kernel(
    sizes, sol_in, res_in, dir_in, img_in, gram_in, sol_out, res_out, dir_out,
    sol, res, prev, prev_img, gram, land, strip, halo, done, back, part, parts, early, earlies,
    local_sem, send_sem, recv_sem,
):
    ngx, ngy, ngz, n, lx, lz, width = sizes
    s, level = lx * lz, ngz // 2
    per = n // (ngx * level)
    some = per * s
    gx, gy, gz = lax.axis_index("gx"), lax.axis_index("gy"), lax.axis_index("gz")
    column = gx * ngz + gz
    place = gy * n + column
    everyone = n * ngy

    loads = [
        pltpu.make_async_copy(a, b, local_sem.at[i])
        for i, (a, b) in enumerate(
            ((res_in, res), (gram_in, gram), (dir_in, prev), (img_in, prev_img), (sol_in, sol))
        )
    ]
    for load in loads:
        load.start()

    low = gz < level
    floors = [
        jnp.where(
            low,
            jnp.where(ngz - 1 - k > gz, ngz - 1 - k, ngz - 2 - k),
            jnp.where(k < gz, k, k + 1),
        )
        for k in range(ngz - 1)
    ] + [gz]
    across = [jnp.bitwise_xor(gx, dx) for dx in range(ngx)]
    ways = sorted(
        ((dx, dy, k) for dx in range(ngx) for dy in range(ngy) for k in range(ngz)),
        key=lambda way: (way[2] >= level, way[2] - (way[0] > 1) - way[1], -way[1], -way[0]),
    )
    flock = []
    for dx, dy, k in ways:
        if (dx, dy, k) != (0, 0, ngz - 1):
            ox, oy, oz = across[dx], 1 - gy if dy else gy, floors[k]
            owner = ox * level + jnp.bitwise_and(oz, level - 1)
            flock.append((dy == 0, k >= level, owner, ox * ngz + oz, {"gx": ox, "gy": oy, "gz": oz}))
    owner = gx * level + jnp.bitwise_and(gz, level - 1)

    def remote(source, target, sent, arrived, where):
        pltpu.make_async_remote_copy(
            src_ref=source, dst_ref=target, send_sem=send_sem.at[sent], recv_sem=recv_sem.at[arrived],
            device_id=where, device_id_type=MESH,
        ).start()

    def wait(ref, semaphore):
        pltpu.make_async_copy(ref, ref, semaphore).wait()

    land[...] = jnp.zeros_like(land)
    barrier = pltpu.get_barrier_semaphore()
    for peer in flock:
        pl.semaphore_signal(barrier, inc=1, device_id=peer[4], device_id_type=MESH)
    loads[0].wait()
    depth = width // s
    lanes = lax.broadcasted_iota(jnp.int32, (n, width), 1)
    packed = jnp.zeros((n, width), jnp.float32)
    for i in range(s):
        line = res[pl.ds(i, n, stride=s), :]
        line = pltpu.roll(line, lax.rem(i * depth + jnp.where(gy == 0, depth, 0), width), 1)
        packed = jnp.where(lanes // depth == i, line, packed)
    for i in range(n):
        strip[i] = packed[i : i + 1, :]
    pl.semaphore_wait(barrier, everyone - 1)

    mine = land.at[pl.ds(column * some, some), :]
    spans = spans_of(ngz, lx, lz)

    def by_plane(work):
        for span in sorted(set(spans)):
            here = functools.reduce(jnp.logical_or, [gz == g for g in range(ngz) if spans[g] == span])
            pl.when(here)(functools.partial(work, *span))

    def cross(begin, end):
        for same, level_with, into, _, where in flock:
            if same and not level_with:
                remote(
                    res.reshape(n, s, width).at[pl.ds(into * per, per), pl.ds(begin, end - begin), :],
                    land.reshape(per * n, s, width).at[pl.ds(column * per, per), pl.ds(begin, end - begin), :],
                    6, 8, where,
                )

    def edges(level_with_me):
        for same, level_with, into, _, where in flock:
            if not same and level_with == level_with_me:
                remote(strip.at[pl.ds(into * per, per)], halo.at[pl.ds(column * per, per)], 5, 1, where)

    edges(False)
    by_plane(cross)
    edges(True)
    for same, level_with, into, _, where in flock:
        if same and level_with:
            remote(res.at[pl.ds(into * some, some), :], mine, 0, 0, where)
    pltpu.make_async_copy(res.at[pl.ds(owner * some, some), :], mine, recv_sem.at[0]).start()

    def flat(ref, first, stride):
        return jnp.concatenate([ref[pl.ds(first + i, n, stride=stride), :] for i in range(s)], axis=1)

    def send_all(source, target, sent, arrived):
        for peer in flock:
            remote(source, target, sent, arrived, peer[4])
        pltpu.make_async_copy(source, target, recv_sem.at[arrived]).start()

    planes = [(x, z) for x in range(lx) for z in range(lz)]
    for load in loads[1:4]:
        load.wait()
    p, q = flat(prev, 0, s), flat(prev_img, 0, s)
    q_parts = parts_of(q)
    early[0] = pack(gram_of(parts_of(p), q_parts))
    eye = (lax.broadcasted_iota(jnp.int32, (n, n), 0) == lax.broadcasted_iota(jnp.int32, (n, n), 1)).astype(jnp.float32)
    inverse = eliminate(0.5 * (gram[...] + gram[...].T), eye)

    wait(land.at[pl.ds(0, level * ngx * some), :], recv_sem.at[0])
    above = ngx * per * sum(end - begin for begin, end in spans[level:])
    below = ngx * per * sum(end - begin for begin, end in spans[:level])

    @pl.when(low)
    def _():
        wait(land.at[pl.ds(0, above), :], recv_sem.at[8])

    @pl.when(jnp.logical_not(low))
    def _():
        wait(land.at[pl.ds(0, below), :], recv_sem.at[8])


    lines = {(x, z): [land[pl.ds(a * s + x * lz + z, n, stride=some), :] for a in range(per)] for x, z in planes}
    sweeps = [
        smooth([[lines[x, z][a] for z in range(lz)] for x in range(lx)], ngx, ngz, gy, True) for a in range(per)
    ]
    begun = [[next(sweep) for _ in range(2)] for sweep in sweeps]
    wait(halo, recv_sem.at[1])
    beyond = [jnp.concatenate([halo[i * per + a] for i in range(n)], axis=0) for a in range(per)]
    zone = width // per
    outer = jnp.where(gy == 0, zone - depth, 0)
    shift = jnp.where(gy == 0, zone, depth)

    def border_of(x, z):
        i = x * lz + z
        edge = None
        for a in range(per):
            begin = a * zone
            inside = pltpu.roll(lines[x, z][a], lax.rem(begin + shift + jnp.where(gy == 0, width - depth, 0), width), 1)
            outside = pltpu.roll(beyond[a], lax.rem(begin + outer + width - i * depth, width), 1)
            at = lanes - (begin + outer)
            value = jnp.where(jnp.logical_and(at >= 0, at < depth), outside, inside)
            edge = value if edge is None else jnp.where(lanes >= begin, value, edge)
        return edge

    border = jnp.where(gy == 0, width - depth, 0)
    at_border = jnp.logical_and(lanes >= border, lanes < border + depth)

    def keep(field, values, odd=None):
        for i, (x, z) in enumerate(planes):
            if odd is not None and x % 2 != odd:
                continue
            edge = values[per][x, z]
            for a in range(per):
                back_shift = lax.rem(2 * width - a * zone - shift - jnp.where(gy == 0, width - depth, 0), width)
                value = jnp.where(at_border, pltpu.roll(edge, back_shift, 1), values[a][x, z])
                done[field, pl.ds(a * s + i, n, stride=some), :] = value
        source, target = (ref.at[field].reshape(ref.shape[1] // s, s, width) for ref in (done, back))
        rows = pl.ds(0, s) if odd is None else pl.ds(odd * (s // 2), s // 2)
        target = target.at[pl.ds(owner * per, per), rows, :]
        for same, level_with, _, home, where in flock:
            if same and level_with:
                remote(source.at[pl.ds(home * per, per), rows, :], target, 1, 2 + field, where)
        pltpu.make_async_copy(source.at[pl.ds(column * per, per), rows, :], target, recv_sem.at[2 + field]).start()

    edge_rows = [[border_of(x, z) for z in range(lz)] for x in range(lx)]
    sweeps.append(smooth(edge_rows, ngx, ngz, gy, False))
    begun.append([])
    for step in range(8):
        found = [past[step] if step < len(past) else next(sweep) for past, sweep in zip(begun, sweeps)]
        if step in (1, 3):
            keep(0, [forward for forward, _ in found], step // 2)
        if step in (4, 6):
            keep(1, [state for _, state in found], 1 if step == 4 else 0)
    keep(2, [image for image, _ in found])
    send_all(early.at[0], earlies.at[0, place], 2, 5)

    wait(back.at[0], recv_sem.at[2])
    yf = flat(back.at[0], 0, s)
    y_parts = parts_of(yf)
    early[1] = pack(26.0 * gram_of(y_parts, y_parts))
    send_all(early.at[1], earlies.at[1, place], 3, 6)

    wait(back.at[1], recv_sem.at[3])
    zf = flat(back.at[1], 0, s)
    uf = zf - yf
    u_parts = parts_of(uf)
    part[...] = pack(jnp.concatenate([gram_of(u_parts, u_parts), gram_of(parts_of(zf), q_parts)], axis=1))
    send_all(part, parts.at[place], 4, 7)

    def summed(ref):
        return tree_sum([ref[i] for i in range(everyone)])

    wait(earlies.at[0], recv_sem.at[5])
    middle = dot(dot(inverse, unpack(summed(earlies.at[0]), n)), inverse)
    pair_parts = parts_of(jnp.concatenate([inverse, middle], axis=0))
    wait(earlies.at[1], recv_sem.at[6])
    gram_zr = unpack(summed(earlies.at[1]), n)
    zr_parts = parts_of(gram_zr)
    found = product(pair_parts, zr_parts, ((1,), (0,)))
    beta, inner = found[:n], found[n:]
    known = gram_zr + product(zr_parts, parts_of(inner), ((1,), (0,)))
    blocks = 128 // (2 * n)
    right_parts = parts_of(jnp.concatenate([-26.0 * eye, beta] * blocks, axis=0))
    left_parts = parts_of(jnp.concatenate([0.0 * eye, beta] * blocks, axis=0).T)
    row, lane = (lax.broadcasted_iota(jnp.int32, (n, 128), i) for i in range(2))
    mine_only = row // (n // blocks) == lane // (2 * n)
    mixed = wide(beta, parts_of(jnp.concatenate([p, q], axis=1)))
    direction = zf + mixed[:, : s * width]
    wait(back.at[2], recv_sem.at[4])
    wf = flat(back.at[2], 0, s)
    both = jnp.concatenate([direction, wf + mixed[:, s * width :]], axis=1)
    both_parts = parts_of(both)
    for i in range(s):
        dir_out[pl.ds(i, n, stride=s), :] = direction[:, i * width : (i + 1) * width]
    loads[4].wait()
    wait(land.at[pl.ds(0, (level * ngx - 1) * some), :], send_sem.at[0])
    by_plane(lambda begin, end: wait(land.at[pl.ds(0, level * ngx * per * (end - begin)), :], send_sem.at[6]))
    wait(halo, send_sem.at[5])
    wait(back.at[pl.ds(0, 3), pl.ds(0, (n // per - 1) * some), :], send_sem.at[1])
    wait(earlies.at[0, pl.ds(0, everyone - 1)], send_sem.at[2])
    wait(earlies.at[1, pl.ds(0, everyone - 1)], send_sem.at[3])

    wait(parts, recv_sem.at[7])
    total = parts_of(jnp.where(mine_only, jnp.concatenate([summed(parts)] * blocks, axis=0), 0.0))
    curvature = known + product(total, right_parts, ((1,), (0,))) + gram_of(left_parts, total)
    alpha = eliminate(curvature, gram_zr)
    step = wide(alpha, both_parts)
    for i in range(s):
        rows = pl.ds(i, n, stride=s)
        sol_out[rows, :] = sol[rows, :] + step[:, i * width : (i + 1) * width]
        res_out[rows, :] = res[rows, :] - step[:, (s + i) * width : (s + i + 1) * width]
    wait(parts.at[pl.ds(0, everyone - 1)], send_sem.at[4])


def write(*refs):
    half = len(refs) // 2
    semaphore = refs[-1]
    stores = [pltpu.make_async_copy(refs[i], refs[half + i], semaphore.at[i]) for i in range(half)]
    for store in stores:
        store.start()
    for store in stores:
        store.wait()


def whole_body(sizes, *args):
    ngx, ngy, ngz, n, lx, lz, width = sizes
    s, everyone = lx * lz, n * ngy
    rows = n * s
    shape = args[0].shape
    field = jax.ShapeDtypeStruct((rows, width), jnp.float32)
    anywhere = pl.BlockSpec(memory_space=pl.ANY)
    inside = pl.BlockSpec(memory_space=pltpu.VMEM)
    block = pltpu.VMEM((rows, width), jnp.float32)
    per = 2 * n // (ngx * ngz)
    packed = n * n // 128
    outs = pl.pallas_call(
        functools.partial(kernel, sizes),
        out_shape=(block,) * 3,
        in_specs=[anywhere] * 5,
        out_specs=[inside] * 3,
        scratch_shapes=[
            block, block, block, block,
            pltpu.VMEM((n, n), jnp.float32),
            pltpu.VMEM((per * rows, width), jnp.float32),
            pltpu.VMEM((n, 1, width), jnp.float32),
            pltpu.VMEM((per * n, 1, width), jnp.float32),
            pltpu.VMEM((3, per * rows, width), jnp.float32),
            pltpu.VMEM((3, rows, width), jnp.float32),
            pltpu.VMEM((2 * packed, 128), jnp.float32),
            pltpu.VMEM((everyone, 2 * packed, 128), jnp.float32),
            pltpu.VMEM((2, packed, 128), jnp.float32),
            pltpu.VMEM((2, everyone, packed, 128), jnp.float32),
            pltpu.SemaphoreType.DMA((5,)),
            pltpu.SemaphoreType.DMA((7,)),
            pltpu.SemaphoreType.DMA((9,)),
        ],
        compiler_params=pltpu.CompilerParams(
            collective_id=0, has_side_effects=True
        ),
    )(*(a.reshape(rows, width) for a in args[:4]), args[4])
    outs = [pltpu.with_memory_space_constraint(a, pltpu.VMEM) for a in outs]
    outs = pl.pallas_call(
        write,
        out_shape=(field,) * 3,
        in_specs=[inside] * 3,
        out_specs=[anywhere] * 3,
        scratch_shapes=[pltpu.SemaphoreType.DMA((3,))],

    )(*outs)
    return tuple(a.reshape(shape) for a in outs)


def pick_body(mesh, solution, residual, direction_prev, image_prev, gram_prev):
    ngx, ngy, ngz = (mesh.shape[axis] for axis in ("gx", "gy", "gz"))
    n, lx, lz, width = residual.shape
    fits = n == ngx * ngz and lx == 2 and lz % 2 == 0 and (lx * lz) % 8 == 0
    fits = fits and width % 128 == 0 and n % 16 == 0 and 128 % (2 * n) == 0 and ngy == 2 and ngz > 1 and width >= 4 * (width // (lx * lz)) and (ngx & (ngx - 1)) == 0 and (ngz & (ngz - 1)) == 0 and width % (lx * lz) == 0 and width // (lx * lz) >= 15
    args = (solution, residual, direction_prev, image_prev, gram_prev)
    if fits:
        return whole_body((ngx, ngy, ngz, n, lx, lz, width), *args)
    return body(*args)


def solution(mesh):
    in_specs = (
        P(None, "gx", "gz", "gy"),
        P(None, "gx", "gz", "gy"),
        P(None, "gx", "gz", "gy"),
        P(None, "gx", "gz", "gy"),
        P(),
    )
    out_specs = (P(None, "gx", "gz", "gy"), P(None, "gx", "gz", "gy"), P(None, "gx", "gz", "gy"))
    return jax.shard_map(functools.partial(pick_body, mesh), mesh=mesh, in_specs=in_specs, out_specs=out_specs, check_vma=False)
```

```python
import functools

import jax
import jax.numpy as jnp
from jax import lax
from jax.experimental import pallas as pl
from jax.experimental.pallas import tpu as pltpu
from jax.sharding import PartitionSpec as P


def with_halo(value, sides, width):
    for axis, dim in sides:
        devices, length = (lax.axis_size(axis), value.shape[dim])
        up = [(i, (i + 1) % devices) for i in range(devices - 1)]
        down = [(j, i) for i, j in up]
        last = lax.slice_in_dim(value, length - width, length, axis=dim)
        first = lax.slice_in_dim(value, 0, width, axis=dim)
        before = lax.ppermute(last, axis, up)
        after = lax.ppermute(first, axis, down)
        value = jnp.concatenate([before, value, after], axis=dim)
    return value


def box_sum(padded):
    total = padded[:, :-2] + padded[:, 1:-1] + padded[:, 2:]
    total = total[:, :, :-2] + total[:, :, 1:-1] + total[:, :, 2:]
    return total[:, :, :, :-2] + total[:, :, :, 1:-1] + total[:, :, :, 2:]


def colors_of(shape):
    first = lax.broadcasted_iota(jnp.int32, shape, 1) % 2
    second = lax.broadcasted_iota(jnp.int32, shape, 2) % 2
    third = lax.broadcasted_iota(jnp.int32, shape, 3) % 2
    return 4 * first + 2 * second + third


def local_gram(left, right):
    return jnp.einsum("kxzy,lxzy->kl", left, right, precision=lax.Precision.HIGHEST)


def combine(field, mixing):
    return jnp.einsum("kxzy,kl->lxzy", field, mixing, precision=lax.Precision.HIGHEST)


def small_dot(left, right):
    return jnp.dot(left, right, precision=lax.Precision.HIGHEST)


def spd_solve(matrix, target):
    order = matrix.shape[0]
    sym = 0.5 * (matrix + matrix.T)
    lower = jnp.zeros_like(sym)
    for col in range(order):
        column = sym[col:, col] - jnp.sum(lower[col:, :col] * lower[col, :col][None, :], axis=1)
        pivot = jnp.sqrt(column[0])
        lower = lower.at[col:, col].set(column / pivot)
    middle = jnp.zeros_like(target)
    for row in range(order):
        value = target[row] - jnp.sum(lower[row, :row][:, None] * middle[:row], axis=0)
        middle = middle.at[row].set(value / lower[row, row])
    answer = jnp.zeros_like(target)
    for row in range(order - 1, -1, -1):
        value = middle[row] - jnp.sum(lower[row + 1 :, row][:, None] * answer[row + 1 :], axis=0)
        answer = answer.at[row].set(value / lower[row, row])
    return answer


def sweep_box(field):
    padded = with_halo(field, (("gx", 1), ("gy", 3), ("gz", 2)), 1)
    return box_sum(padded)


def body(solution, residual, direction_prev, image_prev, gram_prev):
    colors = colors_of(residual.shape)
    smoothed = jnp.where(colors == 0, residual / 26.0, jnp.float32(0.0))
    for shade in list(range(1, 8)) + list(range(6, -1, -1)):
        boxed = sweep_box(smoothed)
        smoothed = jnp.where(colors == shade, (residual + boxed - smoothed) / 26.0, smoothed)
    padded = with_halo(smoothed, (("gx", 1), ("gy", 3), ("gz", 2)), 1)
    image = 27.0 * smoothed - box_sum(padded)
    sums = (
        local_gram(smoothed, residual),
        local_gram(smoothed, image),
        local_gram(smoothed, image_prev),
        local_gram(direction_prev, image),
        local_gram(direction_prev, image_prev),
    )
    gram_zr, gram_zw, gram_zq, gram_pw, gram_pq = lax.psum(
        (sums[0], sums[1], sums[2], sums[3], sums[4]), ("gx", "gy", "gz")
    )
    beta_mix = spd_solve(gram_prev, gram_zr)
    direction = smoothed + combine(direction_prev, beta_mix)
    image_new = image + combine(image_prev, beta_mix)
    curvature = gram_zw + small_dot(gram_zq, beta_mix) + small_dot(beta_mix.T, gram_pw)
    curvature = curvature + small_dot(small_dot(beta_mix.T, gram_pq), beta_mix)
    alpha_step = spd_solve(curvature, gram_zr)
    solution_new = solution + combine(direction, alpha_step)
    residual_new = residual - combine(image_new, alpha_step)
    return (solution_new, residual_new, direction)


MESH = pl.DeviceIdType.MESH
HIGHEST = lax.Precision.HIGHEST


def dot(left, right):
    return jnp.dot(left, right, precision=HIGHEST, preferred_element_type=jnp.float32)


def dot_nt(left, right):
    return lax.dot_general(
        left, right, (((1,), (1,)), ((), ())), precision=HIGHEST, preferred_element_type=jnp.float32
    )


def parts_of(value):
    first = value.astype(jnp.bfloat16)
    rest = value - first.astype(jnp.float32)
    second = rest.astype(jnp.bfloat16)
    third = (rest - second.astype(jnp.float32)).astype(jnp.bfloat16)
    return first, second, third


def product(left, right, contract):
    order = left[0].shape[0]
    total = None
    for i, term in enumerate(right):
        stack = jnp.concatenate(left[: 3 - i], axis=0) if i < 2 else left[0]
        out = lax.dot_general(stack, term, (contract, ((), ())), preferred_element_type=jnp.float32)
        for j in range(3 - i):
            piece = out[j * order : (j + 1) * order]
            total = piece if total is None else total + piece
    return total


def gram_of(left, right):
    return product(left, right, ((1,), (1,)))


def small(left, right):
    return product(parts_of(left), parts_of(right), ((1,), (0,)))


def wide(turned, right):
    a, b, c = (v.astype(jnp.float32) for v in parts_of(turned))
    d, e, f = right
    left = jnp.concatenate([a, a, b, b, a, c], axis=0).T.astype(jnp.bfloat16)
    return jnp.dot(left, jnp.concatenate([d, e, d, e, f, d], axis=0), preferred_element_type=jnp.float32)


def eliminate(matrix, target):
    order = matrix.shape[0]
    rows = lax.broadcasted_iota(jnp.int32, matrix.shape, 0)
    columns = [jnp.broadcast_to(matrix[:, k : k + 1], matrix.shape) for k in range(order)]
    scale = jnp.zeros(matrix.shape, jnp.float32)
    for c in range(order):
        inverse = 1.0 / columns[c][c : c + 1, :]
        here = rows == c
        factor = jnp.where(here, 0.0, columns[c] * inverse)
        for k in range(c + 1, order):
            columns[k] = columns[k] - factor * columns[k][c : c + 1, :]
        target = target - factor * target[c : c + 1, :]
        scale = jnp.where(here, inverse, scale)
    return target * scale


def smooth(res, ngx, ngz, gy, ends):
    lx, lz = len(res), len(res[0])
    count, ny = res[0][0].shape
    row = lax.broadcasted_iota(jnp.int32, (count, ny), 0)
    lane = lax.broadcasted_iota(jnp.int32, (count, ny), 1)
    even = lane % 2 == 0
    edges = {
        "xp": (row < ngz, ngz),
        "xn": (row >= (ngx - 1) * ngz, count - ngz),
        "zp": (row % ngz == 0, 1),
        "zn": (row % ngz == ngz - 1, count - 1),
    }
    odd = jnp.logical_not(even)
    if ends:
        first, last = jnp.where(gy == 0, 0, -8), jnp.where(gy == 0, -8, ny - 1)
        cut = jnp.where(gy == 0, ny - 3, 0)
        valid = jnp.logical_or(lane < cut, lane > cut + 2)
        valid_even, valid_odd = jnp.logical_and(valid, even), jnp.logical_and(valid, odd)
        twice = 2.0 - jnp.where(jnp.logical_or(lane == first, lane == last), 1.0, 0.0)
        below = 3.0 - jnp.where(jnp.logical_or(lane == first + 1, lane == last), 1.0, 0.0)
        above = 3.0 - jnp.where(jnp.logical_or(lane == last - 1, lane == first), 1.0, 0.0)
    else:
        twice, below, above = jnp.float32(2.0), jnp.float32(3.0), jnp.float32(3.0)
    zero = jnp.zeros((count, ny), jnp.float32)
    memo = {}

    def moved(value, kind):
        if value is None:
            return None
        key = (kind, id(value))
        if key not in memo:
            edge, amount = edges[kind]
            memo[key] = (value, jnp.where(edge, zero, pltpu.roll(value, amount, 0)))
        return memo[key][1]

    def add(*values):
        total = None
        for value in values:
            if value is not None:
                total = value if total is None else total + value
        return total

    state = {(x, z): None for x in range(lx) for z in range(lz)}

    def z_pair(x, z):
        before = state[x, z - 1] if z > 0 else moved(state[x, lz - 1], "zp")
        after = state[x, z + 1] if z < lz - 1 else moved(state[x, 0], "zn")
        return add(before, after)

    def neighbours(x, z):
        def line(other):
            return add(state[other, z], z_pair(other, z))

        before = line(x - 1) if x > 0 else moved_line(lx - 1, z, "xp")
        after = line(x + 1) if x < lx - 1 else moved_line(0, z, "xn")
        return add(z_pair(x, z), before, after)

    def moved_line(x, z, kind):
        return moved(add(state[x, z], z_pair(x, z)), kind)

    def woven(at_even, at_odd):
        if not ends:
            return jnp.where(even, at_even, at_odd)
        return jnp.where(valid_even, at_even, jnp.where(valid_odd, at_odd, zero))

    def shifted(value, k):
        return pltpu.roll(value, k, 1), pltpu.roll(value, ny - k, 1)

    def once(value):
        return sum(shifted(value, 1))

    def two(value):
        return sum(shifted(value, 2)) + twice * value

    third = jnp.float32(1.0 / 26.0)
    plan = [(0, 0), (0, 1), (1, 0), (1, 1), (1, 0), (0, 1), (0, 0)]
    forward = {}
    for step, (xp, zp) in enumerate(plan):
        fresh = {}
        for x in range(xp, lx, 2):
            for z in range(zp, lz, 2):
                near, value = neighbours(x, z), state[x, z]
                own = res[x][z]
                both = own if near is None else own + near
                share = third * both
                if value is None and near is None:
                    fresh[x, z] = jnp.where(even, share, third * (own + once(woven(share, zero))))
                    forward[x, z] = fresh[x, z]
                elif value is None:
                    mix = woven(near + share, near)
                    down, up = shifted(mix, 1)
                    pair, far = down + up, two(mix)
                    base = both + pair
                    later = third * (base + third * far)
                    fresh[x, z] = forward[x, z] = jnp.where(even, third * base, later)
                    if step == 3:
                        deep = sum(shifted(mix, 3)) + below * down + above * up
                        again = base + third * (once(woven(zero, both)) + far + third * deep)
                        fresh[x, z] = jnp.where(even, third * again, later)
                else:
                    mix = woven(near + value, near + share)
                    base = both + once(mix)
                    fresh[x, z] = third * jnp.where(even, base + third * two(mix), base)
        state.update(fresh)
        yield forward, state
    image = {}
    for x in range(lx):
        for z in range(lz):
            box = add(state[x, z], neighbours(x, z))
            image[x, z] = 27.0 * state[x, z] - (box + once(jnp.where(valid, box, zero) if ends else box))
    yield image, None


def pack(value):
    rows = value.shape[0] * value.shape[1] // 128
    return jnp.concatenate([value[i : i + rows] for i in range(0, value.shape[0], rows)], axis=1)


def unpack(value, lanes):
    return jnp.concatenate([value[:, i : i + lanes] for i in range(0, value.shape[1], lanes)], axis=0)


def tree_sum(values):
    while len(values) > 1:
        values = [sum(values[i + 1 : i + 2], values[i]) for i in range(0, len(values), 2)]
    return values[0]


def spans_of(ngz, lx, lz):
    level, spans = ngz // 2, []
    for plane in range(ngz):
        rows = []
        for x in range(lx):
            for z in range(lz):
                below = level * lz - 1 - (plane * lz + z)
                away, reach = (below, 5) if below >= 0 else (-1 - below, 6)
                if away <= reach - 2 * (x % 2):
                    rows.append(x * lz + z)
        spans.append((rows[0], rows[-1] + 1) if rows else (0, 0))
    return spans


def kernel(
    sizes, sol_in, res_in, dir_in, img_in, gram_in, sol_out, res_out, dir_out,
    sol, res, prev, prev_img, gram, land, strip, halo, done, back, part, parts, early, earlies,
    local_sem, send_sem, recv_sem,
):
    ngx, ngy, ngz, n, lx, lz, width = sizes
    s, level = lx * lz, ngz // 2
    per = n // (ngx * level)
    some = per * s
    gx, gy, gz = lax.axis_index("gx"), lax.axis_index("gy"), lax.axis_index("gz")
    column = gx * ngz + gz
    place = gy * n + column
    everyone = n * ngy

    loads = [
        pltpu.make_async_copy(a, b, local_sem.at[i])
        for i, (a, b) in enumerate(
            ((res_in, res), (gram_in, gram), (dir_in, prev), (img_in, prev_img), (sol_in, sol))
        )
    ]
    for load in loads:
        load.start()

    low = gz < level
    floors = [
        jnp.where(
            low,
            jnp.where(ngz - 1 - k > gz, ngz - 1 - k, ngz - 2 - k),
            jnp.where(k < gz, k, k + 1),
        )
        for k in range(ngz - 1)
    ] + [gz]
    chip = gx - jnp.bitwise_and(gx, 1)
    across = [jnp.bitwise_xor(chip, dx) for dx in range(ngx)]
    ways = sorted(
        ((dx, dy, k) for dx in range(ngx) for dy in range(ngy) for k in range(ngz)),
        key=lambda way: (way[2] >= level, way[0] % 2, -way[1], way[2] - (way[0] > 1)),
    )
    flock = []
    for dx, dy, k in ways:
        if (dx, dy, k) != (0, 0, ngz - 1):
            ox, oy, oz = across[dx], 1 - gy if dy else gy, floors[k]
            if (dx, dy, k) == (1, 0, ngz - 1):
                ox = jnp.bitwise_xor(gx, 1)
            into = ox * level + jnp.bitwise_and(oz, level - 1)
            flock.append((dy == 0, k >= level, into, ox * ngz + oz, {"gx": ox, "gy": oy, "gz": oz}))
    owner = gx * level + jnp.bitwise_and(gz, level - 1)

    def remote(source, target, sent, arrived, where):
        pltpu.make_async_remote_copy(
            src_ref=source, dst_ref=target, send_sem=send_sem.at[sent], recv_sem=recv_sem.at[arrived],
            device_id=where, device_id_type=MESH,
        ).start()

    def wait(ref, semaphore):
        pltpu.make_async_copy(ref, ref, semaphore).wait()

    land[...] = jnp.zeros_like(land)
    barrier = pltpu.get_barrier_semaphore()
    for peer in flock:
        pl.semaphore_signal(barrier, inc=1, device_id=peer[4], device_id_type=MESH)
    loads[0].wait()
    depth = width // s
    lanes = lax.broadcasted_iota(jnp.int32, (n, width), 1)
    packed = jnp.zeros((n, width), jnp.float32)
    for i in range(s):
        line = res[pl.ds(i, n, stride=s), :]
        line = pltpu.roll(line, lax.rem(i * depth + jnp.where(gy == 0, depth, 0), width), 1)
        packed = jnp.where(lanes // depth == i, line, packed)
    for i in range(n):
        strip[i] = packed[i : i + 1, :]
    pl.semaphore_wait(barrier, everyone - 1)

    mine = land.at[pl.ds(column * some, some), :]
    spans = spans_of(ngz, lx, lz)

    def by_plane(work):
        for span in sorted(set(spans)):
            here = functools.reduce(jnp.logical_or, [gz == g for g in range(ngz) if spans[g] == span])
            pl.when(here)(functools.partial(work, *span))

    def cross(begin, end):
        for same, level_with, into, _, where in flock:
            if same and not level_with:
                remote(
                    res.reshape(n, s, width).at[pl.ds(into * per, per), pl.ds(begin, end - begin), :],
                    land.reshape(per * n, s, width).at[pl.ds(column * per, per), pl.ds(begin, end - begin), :],
                    6, 8, where,
                )

    def edges(level_with_me):
        for same, level_with, into, _, where in flock:
            if not same and level_with == level_with_me:
                remote(strip.at[pl.ds(into * per, per)], halo.at[pl.ds(column * per, per)], 5, 1, where)

    edges(False)
    by_plane(cross)
    edges(True)
    for same, level_with, into, _, where in flock:
        if same and level_with:
            remote(res.at[pl.ds(into * some, some), :], mine, 0, 0, where)
    pltpu.make_async_copy(res.at[pl.ds(owner * some, some), :], mine, recv_sem.at[0]).start()

    def flat(ref, first, stride):
        return jnp.concatenate([ref[pl.ds(first + i, n, stride=stride), :] for i in range(s)], axis=1)

    def send_all(source, target, sent, arrived):
        for peer in flock:
            remote(source, target, sent, arrived, peer[4])
        pltpu.make_async_copy(source, target, recv_sem.at[arrived]).start()

    planes = [(x, z) for x in range(lx) for z in range(lz)]
    for load in loads[1:4]:
        load.wait()
    p, q = flat(prev, 0, s), flat(prev_img, 0, s)
    q_parts = parts_of(q)
    early[0] = pack(gram_of(parts_of(p), q_parts))
    eye = (lax.broadcasted_iota(jnp.int32, (n, n), 0) == lax.broadcasted_iota(jnp.int32, (n, n), 1)).astype(jnp.float32)
    inverse = eliminate(0.5 * (gram[...] + gram[...].T), eye)

    wait(land.at[pl.ds(0, level * ngx * some), :], recv_sem.at[0])
    above = ngx * per * sum(end - begin for begin, end in spans[level:])
    below = ngx * per * sum(end - begin for begin, end in spans[:level])

    @pl.when(low)
    def _():
        wait(land.at[pl.ds(0, above), :], recv_sem.at[8])

    @pl.when(jnp.logical_not(low))
    def _():
        wait(land.at[pl.ds(0, below), :], recv_sem.at[8])


    lines = {(x, z): [land[pl.ds(a * s + x * lz + z, n, stride=some), :] for a in range(per)] for x, z in planes}
    sweeps = [
        smooth([[lines[x, z][a] for z in range(lz)] for x in range(lx)], ngx, ngz, gy, True) for a in range(per)
    ]
    begun = [[next(sweep) for _ in range(2)] for sweep in sweeps]
    wait(halo, recv_sem.at[1])
    beyond = [jnp.concatenate([halo[i * per + a] for i in range(n)], axis=0) for a in range(per)]
    zone = width // per
    outer = jnp.where(gy == 0, zone - depth, 0)
    shift = jnp.where(gy == 0, zone, depth)

    def border_of(x, z):
        i = x * lz + z
        edge = None
        for a in range(per):
            begin = a * zone
            inside = pltpu.roll(lines[x, z][a], lax.rem(begin + shift + jnp.where(gy == 0, width - depth, 0), width), 1)
            outside = pltpu.roll(beyond[a], lax.rem(begin + outer + width - i * depth, width), 1)
            at = lanes - (begin + outer)
            value = jnp.where(jnp.logical_and(at >= 0, at < depth), outside, inside)
            edge = value if edge is None else jnp.where(lanes >= begin, value, edge)
        return edge

    border = jnp.where(gy == 0, width - depth, 0)
    at_border = jnp.logical_and(lanes >= border, lanes < border + depth)

    def keep(field, values, odd=None):
        for i, (x, z) in enumerate(planes):
            if odd is not None and x % 2 != odd:
                continue
            edge = values[per][x, z]
            for a in range(per):
                back_shift = lax.rem(2 * width - a * zone - shift - jnp.where(gy == 0, width - depth, 0), width)
                value = jnp.where(at_border, pltpu.roll(edge, back_shift, 1), values[a][x, z])
                done[field, pl.ds(a * s + i, n, stride=some), :] = value
        source, target = (ref.at[field].reshape(ref.shape[1] // s, s, width) for ref in (done, back))
        rows = pl.ds(0, s) if odd is None else pl.ds(odd * (s // 2), s // 2)
        target = target.at[pl.ds(owner * per, per), rows, :]
        for same, level_with, _, home, where in flock:
            if same and level_with:
                remote(source.at[pl.ds(home * per, per), rows, :], target, 1, 2 + field, where)
        pltpu.make_async_copy(source.at[pl.ds(column * per, per), rows, :], target, recv_sem.at[2 + field]).start()

    edge_rows = [[border_of(x, z) for z in range(lz)] for x in range(lx)]
    sweeps.append(smooth(edge_rows, ngx, ngz, gy, False))
    begun.append([])
    for step in range(8):
        found = [past[step] if step < len(past) else next(sweep) for past, sweep in zip(begun, sweeps)]
        if step in (1, 3):
            keep(0, [forward for forward, _ in found], step // 2)
        if step in (4, 6):
            keep(1, [state for _, state in found], 1 if step == 4 else 0)
    keep(2, [image for image, _ in found])
    send_all(early.at[0], earlies.at[0, place], 2, 5)

    wait(back.at[0], recv_sem.at[2])
    yf = flat(back.at[0], 0, s)
    y_parts = parts_of(yf)
    early[1] = pack(26.0 * gram_of(y_parts, y_parts))
    send_all(early.at[1], earlies.at[1, place], 3, 6)

    wait(back.at[1], recv_sem.at[3])
    zf = flat(back.at[1], 0, s)
    uf = zf - yf
    u_parts = parts_of(uf)
    part[...] = pack(jnp.concatenate([gram_of(u_parts, u_parts), gram_of(parts_of(zf), q_parts)], axis=1))
    send_all(part, parts.at[place], 4, 7)

    def summed(ref):
        return tree_sum([ref[i] for i in range(everyone)])

    wait(earlies.at[0], recv_sem.at[5])
    middle = dot(dot(inverse, unpack(summed(earlies.at[0]), n)), inverse)
    pair_parts = parts_of(jnp.concatenate([inverse, middle], axis=0))
    wait(earlies.at[1], recv_sem.at[6])
    gram_zr = unpack(summed(earlies.at[1]), n)
    zr_parts = parts_of(gram_zr)
    found = product(pair_parts, zr_parts, ((1,), (0,)))
    beta, inner = found[:n], found[n:]
    known = gram_zr + product(zr_parts, parts_of(inner), ((1,), (0,)))
    blocks = 128 // (2 * n)
    right_parts = parts_of(jnp.concatenate([-26.0 * eye, beta] * blocks, axis=0))
    left_parts = parts_of(jnp.concatenate([0.0 * eye, beta] * blocks, axis=0).T)
    row, lane = (lax.broadcasted_iota(jnp.int32, (n, 128), i) for i in range(2))
    mine_only = row // (n // blocks) == lane // (2 * n)
    mixed = wide(beta, parts_of(jnp.concatenate([p, q], axis=1)))
    direction = zf + mixed[:, : s * width]
    wait(back.at[2], recv_sem.at[4])
    wf = flat(back.at[2], 0, s)
    both = jnp.concatenate([direction, wf + mixed[:, s * width :]], axis=1)
    both_parts = parts_of(both)
    for i in range(s):
        dir_out[pl.ds(i, n, stride=s), :] = direction[:, i * width : (i + 1) * width]
    loads[4].wait()
    wait(land.at[pl.ds(0, (level * ngx - 1) * some), :], send_sem.at[0])
    by_plane(lambda begin, end: wait(land.at[pl.ds(0, level * ngx * per * (end - begin)), :], send_sem.at[6]))
    wait(halo, send_sem.at[5])
    wait(back.at[pl.ds(0, 3), pl.ds(0, (n // per - 1) * some), :], send_sem.at[1])
    wait(earlies.at[0, pl.ds(0, everyone - 1)], send_sem.at[2])
    wait(earlies.at[1, pl.ds(0, everyone - 1)], send_sem.at[3])

    wait(parts, recv_sem.at[7])
    total = parts_of(jnp.where(mine_only, jnp.concatenate([summed(parts)] * blocks, axis=0), 0.0))
    curvature = known + product(total, right_parts, ((1,), (0,))) + gram_of(left_parts, total)
    alpha = eliminate(curvature, gram_zr)
    step = wide(alpha, both_parts)
    for i in range(s):
        rows = pl.ds(i, n, stride=s)
        sol_out[rows, :] = sol[rows, :] + step[:, i * width : (i + 1) * width]
        res_out[rows, :] = res[rows, :] - step[:, (s + i) * width : (s + i + 1) * width]
    wait(parts.at[pl.ds(0, everyone - 1)], send_sem.at[4])


def write(*refs):
    half = len(refs) // 2
    semaphore = refs[-1]
    stores = [pltpu.make_async_copy(refs[i], refs[half + i], semaphore.at[i]) for i in range(half)]
    for store in stores:
        store.start()
    for store in stores:
        store.wait()


def whole_body(sizes, *args):
    ngx, ngy, ngz, n, lx, lz, width = sizes
    s, everyone = lx * lz, n * ngy
    rows = n * s
    shape = args[0].shape
    field = jax.ShapeDtypeStruct((rows, width), jnp.float32)
    anywhere = pl.BlockSpec(memory_space=pl.ANY)
    inside = pl.BlockSpec(memory_space=pltpu.VMEM)
    block = pltpu.VMEM((rows, width), jnp.float32)
    per = 2 * n // (ngx * ngz)
    packed = n * n // 128
    outs = pl.pallas_call(
        functools.partial(kernel, sizes),
        out_shape=(block,) * 3,
        in_specs=[anywhere] * 5,
        out_specs=[inside] * 3,
        scratch_shapes=[
            block, block, block, block,
            pltpu.VMEM((n, n), jnp.float32),
            pltpu.VMEM((per * rows, width), jnp.float32),
            pltpu.VMEM((n, 1, width), jnp.float32),
            pltpu.VMEM((per * n, 1, width), jnp.float32),
            pltpu.VMEM((3, per * rows, width), jnp.float32),
            pltpu.VMEM((3, rows, width), jnp.float32),
            pltpu.VMEM((2 * packed, 128), jnp.float32),
            pltpu.VMEM((everyone, 2 * packed, 128), jnp.float32),
            pltpu.VMEM((2, packed, 128), jnp.float32),
            pltpu.VMEM((2, everyone, packed, 128), jnp.float32),
            pltpu.SemaphoreType.DMA((5,)),
            pltpu.SemaphoreType.DMA((7,)),
            pltpu.SemaphoreType.DMA((9,)),
        ],
        compiler_params=pltpu.CompilerParams(
            collective_id=0, has_side_effects=True
        ),
    )(*(a.reshape(rows, width) for a in args[:4]), args[4])
    outs = [pltpu.with_memory_space_constraint(a, pltpu.VMEM) for a in outs]
    outs = pl.pallas_call(
        write,
        out_shape=(field,) * 3,
        in_specs=[inside] * 3,
        out_specs=[anywhere] * 3,
        scratch_shapes=[pltpu.SemaphoreType.DMA((3,))],

    )(*outs)
    return tuple(a.reshape(shape) for a in outs)


def pick_body(mesh, solution, residual, direction_prev, image_prev, gram_prev):
    ngx, ngy, ngz = (mesh.shape[axis] for axis in ("gx", "gy", "gz"))
    n, lx, lz, width = residual.shape
    fits = n == ngx * ngz and lx == 2 and lz % 2 == 0 and (lx * lz) % 8 == 0
    fits = fits and width % 128 == 0 and n % 16 == 0 and 128 % (2 * n) == 0 and ngy == 2 and ngz > 1 and width >= 4 * (width // (lx * lz)) and (ngx & (ngx - 1)) == 0 and (ngz & (ngz - 1)) == 0 and width % (lx * lz) == 0 and width // (lx * lz) >= 15
    args = (solution, residual, direction_prev, image_prev, gram_prev)
    if fits:
        return whole_body((ngx, ngy, ngz, n, lx, lz, width), *args)
    return body(*args)


def solution(mesh):
    in_specs = (
        P(None, "gx", "gz", "gy"),
        P(None, "gx", "gz", "gy"),
        P(None, "gx", "gz", "gy"),
        P(None, "gx", "gz", "gy"),
        P(),
    )
    out_specs = (P(None, "gx", "gz", "gy"), P(None, "gx", "gz", "gy"), P(None, "gx", "gz", "gy"))
    return jax.shard_map(functools.partial(pick_body, mesh), mesh=mesh, in_specs=in_specs, out_specs=out_specs, check_vma=False)
```

```python
import functools

import jax
import jax.numpy as jnp
from jax import lax
from jax.experimental import pallas as pl
from jax.experimental.pallas import tpu as pltpu
from jax.sharding import PartitionSpec as P


def with_halo(value, sides, width):
    for axis, dim in sides:
        devices, length = (lax.axis_size(axis), value.shape[dim])
        up = [(i, (i + 1) % devices) for i in range(devices - 1)]
        down = [(j, i) for i, j in up]
        last = lax.slice_in_dim(value, length - width, length, axis=dim)
        first = lax.slice_in_dim(value, 0, width, axis=dim)
        before = lax.ppermute(last, axis, up)
        after = lax.ppermute(first, axis, down)
        value = jnp.concatenate([before, value, after], axis=dim)
    return value


def box_sum(padded):
    total = padded[:, :-2] + padded[:, 1:-1] + padded[:, 2:]
    total = total[:, :, :-2] + total[:, :, 1:-1] + total[:, :, 2:]
    return total[:, :, :, :-2] + total[:, :, :, 1:-1] + total[:, :, :, 2:]


def colors_of(shape):
    first = lax.broadcasted_iota(jnp.int32, shape, 1) % 2
    second = lax.broadcasted_iota(jnp.int32, shape, 2) % 2
    third = lax.broadcasted_iota(jnp.int32, shape, 3) % 2
    return 4 * first + 2 * second + third


def local_gram(left, right):
    return jnp.einsum("kxzy,lxzy->kl", left, right, precision=lax.Precision.HIGHEST)


def combine(field, mixing):
    return jnp.einsum("kxzy,kl->lxzy", field, mixing, precision=lax.Precision.HIGHEST)


def small_dot(left, right):
    return jnp.dot(left, right, precision=lax.Precision.HIGHEST)


def spd_solve(matrix, target):
    order = matrix.shape[0]
    sym = 0.5 * (matrix + matrix.T)
    lower = jnp.zeros_like(sym)
    for col in range(order):
        column = sym[col:, col] - jnp.sum(lower[col:, :col] * lower[col, :col][None, :], axis=1)
        pivot = jnp.sqrt(column[0])
        lower = lower.at[col:, col].set(column / pivot)
    middle = jnp.zeros_like(target)
    for row in range(order):
        value = target[row] - jnp.sum(lower[row, :row][:, None] * middle[:row], axis=0)
        middle = middle.at[row].set(value / lower[row, row])
    answer = jnp.zeros_like(target)
    for row in range(order - 1, -1, -1):
        value = middle[row] - jnp.sum(lower[row + 1 :, row][:, None] * answer[row + 1 :], axis=0)
        answer = answer.at[row].set(value / lower[row, row])
    return answer


def sweep_box(field):
    padded = with_halo(field, (("gx", 1), ("gy", 3), ("gz", 2)), 1)
    return box_sum(padded)


def body(solution, residual, direction_prev, image_prev, gram_prev):
    colors = colors_of(residual.shape)
    smoothed = jnp.where(colors == 0, residual / 26.0, jnp.float32(0.0))
    for shade in list(range(1, 8)) + list(range(6, -1, -1)):
        boxed = sweep_box(smoothed)
        smoothed = jnp.where(colors == shade, (residual + boxed - smoothed) / 26.0, smoothed)
    padded = with_halo(smoothed, (("gx", 1), ("gy", 3), ("gz", 2)), 1)
    image = 27.0 * smoothed - box_sum(padded)
    sums = (
        local_gram(smoothed, residual),
        local_gram(smoothed, image),
        local_gram(smoothed, image_prev),
        local_gram(direction_prev, image),
        local_gram(direction_prev, image_prev),
    )
    gram_zr, gram_zw, gram_zq, gram_pw, gram_pq = lax.psum(
        (sums[0], sums[1], sums[2], sums[3], sums[4]), ("gx", "gy", "gz")
    )
    beta_mix = spd_solve(gram_prev, gram_zr)
    direction = smoothed + combine(direction_prev, beta_mix)
    image_new = image + combine(image_prev, beta_mix)
    curvature = gram_zw + small_dot(gram_zq, beta_mix) + small_dot(beta_mix.T, gram_pw)
    curvature = curvature + small_dot(small_dot(beta_mix.T, gram_pq), beta_mix)
    alpha_step = spd_solve(curvature, gram_zr)
    solution_new = solution + combine(direction, alpha_step)
    residual_new = residual - combine(image_new, alpha_step)
    return (solution_new, residual_new, direction)


MESH = pl.DeviceIdType.MESH
HIGHEST = lax.Precision.HIGHEST


def dot(left, right):
    return jnp.dot(left, right, precision=HIGHEST, preferred_element_type=jnp.float32)


def dot_nt(left, right):
    return lax.dot_general(
        left, right, (((1,), (1,)), ((), ())), precision=HIGHEST, preferred_element_type=jnp.float32
    )


def parts_of(value):
    first = value.astype(jnp.bfloat16)
    rest = value - first.astype(jnp.float32)
    second = rest.astype(jnp.bfloat16)
    third = (rest - second.astype(jnp.float32)).astype(jnp.bfloat16)
    return first, second, third


def product(left, right, contract):
    order = left[0].shape[0]
    total = None
    for i, term in enumerate(right):
        stack = jnp.concatenate(left[: 3 - i], axis=0) if i < 2 else left[0]
        out = lax.dot_general(stack, term, (contract, ((), ())), preferred_element_type=jnp.float32)
        for j in range(3 - i):
            piece = out[j * order : (j + 1) * order]
            total = piece if total is None else total + piece
    return total


def gram_of(left, right):
    return product(left, right, ((1,), (1,)))


def small(left, right):
    return product(parts_of(left), parts_of(right), ((1,), (0,)))


def wide(turned, right):
    a, b, c = (v.astype(jnp.float32) for v in parts_of(turned))
    d, e, f = right
    left = jnp.concatenate([a, a, b, b, a, c], axis=0).T.astype(jnp.bfloat16)
    return jnp.dot(left, jnp.concatenate([d, e, d, e, f, d], axis=0), preferred_element_type=jnp.float32)


def eliminate(matrix, target):
    order = matrix.shape[0]
    rows = lax.broadcasted_iota(jnp.int32, matrix.shape, 0)
    columns = [jnp.broadcast_to(matrix[:, k : k + 1], matrix.shape) for k in range(order)]
    scale = jnp.zeros(matrix.shape, jnp.float32)
    for c in range(order):
        inverse = 1.0 / columns[c][c : c + 1, :]
        here = rows == c
        factor = jnp.where(here, 0.0, columns[c] * inverse)
        for k in range(c + 1, order):
            columns[k] = columns[k] - factor * columns[k][c : c + 1, :]
        target = target - factor * target[c : c + 1, :]
        scale = jnp.where(here, inverse, scale)
    return target * scale


def smooth(res, ngx, ngz, gy, ends):
    lx, lz = len(res), len(res[0])
    count, ny = res[0][0].shape
    row = lax.broadcasted_iota(jnp.int32, (count, ny), 0)
    lane = lax.broadcasted_iota(jnp.int32, (count, ny), 1)
    even = lane % 2 == 0
    edges = {
        "xp": (row < ngz, ngz),
        "xn": (row >= (ngx - 1) * ngz, count - ngz),
        "zp": (row % ngz == 0, 1),
        "zn": (row % ngz == ngz - 1, count - 1),
    }
    odd = jnp.logical_not(even)
    if ends:
        first, last = jnp.where(gy == 0, 0, -8), jnp.where(gy == 0, -8, ny - 1)
        cut = jnp.where(gy == 0, ny - 3, 0)
        valid = jnp.logical_or(lane < cut, lane > cut + 2)
        valid_even, valid_odd = jnp.logical_and(valid, even), jnp.logical_and(valid, odd)
        twice = 2.0 - jnp.where(jnp.logical_or(lane == first, lane == last), 1.0, 0.0)
        below = 3.0 - jnp.where(jnp.logical_or(lane == first + 1, lane == last), 1.0, 0.0)
        above = 3.0 - jnp.where(jnp.logical_or(lane == last - 1, lane == first), 1.0, 0.0)
    else:
        twice, below, above = jnp.float32(2.0), jnp.float32(3.0), jnp.float32(3.0)
    zero = jnp.zeros((count, ny), jnp.float32)
    memo = {}

    def moved(value, kind):
        if value is None:
            return None
        key = (kind, id(value))
        if key not in memo:
            edge, amount = edges[kind]
            memo[key] = (value, jnp.where(edge, zero, pltpu.roll(value, amount, 0)))
        return memo[key][1]

    def add(*values):
        total = None
        for value in values:
            if value is not None:
                total = value if total is None else total + value
        return total

    state = {(x, z): None for x in range(lx) for z in range(lz)}

    def z_pair(x, z):
        before = state[x, z - 1] if z > 0 else moved(state[x, lz - 1], "zp")
        after = state[x, z + 1] if z < lz - 1 else moved(state[x, 0], "zn")
        return add(before, after)

    def neighbours(x, z):
        def line(other):
            return add(state[other, z], z_pair(other, z))

        before = line(x - 1) if x > 0 else moved_line(lx - 1, z, "xp")
        after = line(x + 1) if x < lx - 1 else moved_line(0, z, "xn")
        return add(z_pair(x, z), before, after)

    def moved_line(x, z, kind):
        return moved(add(state[x, z], z_pair(x, z)), kind)

    def woven(at_even, at_odd):
        if not ends:
            return jnp.where(even, at_even, at_odd)
        return jnp.where(valid_even, at_even, jnp.where(valid_odd, at_odd, zero))

    def shifted(value, k):
        return pltpu.roll(value, k, 1), pltpu.roll(value, ny - k, 1)

    def once(value):
        return sum(shifted(value, 1))

    def two(value):
        return sum(shifted(value, 2)) + twice * value

    third = jnp.float32(1.0 / 26.0)
    plan = [(0, 0), (0, 1), (1, 0), (1, 1), (1, 0), (0, 1), (0, 0)]
    forward = {}
    for step, (xp, zp) in enumerate(plan):
        fresh = {}
        for x in range(xp, lx, 2):
            for z in range(zp, lz, 2):
                near, value = neighbours(x, z), state[x, z]
                own = res[x][z]
                both = own if near is None else own + near
                share = third * both
                if value is None and near is None:
                    fresh[x, z] = jnp.where(even, share, third * (own + once(woven(share, zero))))
                    forward[x, z] = fresh[x, z]
                elif value is None:
                    mix = woven(near + share, near)
                    down, up = shifted(mix, 1)
                    pair, far = down + up, two(mix)
                    base = both + pair
                    later = third * (base + third * far)
                    fresh[x, z] = forward[x, z] = jnp.where(even, third * base, later)
                    if step == 3:
                        deep = sum(shifted(mix, 3)) + below * down + above * up
                        again = base + third * (once(woven(zero, both)) + far + third * deep)
                        fresh[x, z] = jnp.where(even, third * again, later)
                else:
                    mix = woven(near + value, near + share)
                    base = both + once(mix)
                    fresh[x, z] = third * jnp.where(even, base + third * two(mix), base)
        state.update(fresh)
        yield forward, state
    image = {}
    for x in range(lx):
        for z in range(lz):
            box = add(state[x, z], neighbours(x, z))
            image[x, z] = 27.0 * state[x, z] - (box + once(jnp.where(valid, box, zero) if ends else box))
    yield image, None


def pack(value):
    rows = value.shape[0] * value.shape[1] // 128
    return jnp.concatenate([value[i : i + rows] for i in range(0, value.shape[0], rows)], axis=1)


def unpack(value, lanes):
    return jnp.concatenate([value[:, i : i + lanes] for i in range(0, value.shape[1], lanes)], axis=0)


def tree_sum(values):
    while len(values) > 1:
        values = [sum(values[i + 1 : i + 2], values[i]) for i in range(0, len(values), 2)]
    return values[0]


def spans_of(ngz, lx, lz):
    level, spans = ngz // 2, []
    for plane in range(ngz):
        rows = []
        for x in range(lx):
            for z in range(lz):
                below = level * lz - 1 - (plane * lz + z)
                away, reach = (below, 5) if below >= 0 else (-1 - below, 6)
                if away <= reach - 2 * (x % 2):
                    rows.append(x * lz + z)
        spans.append((rows[0], rows[-1] + 1) if rows else (0, 0))
    return spans


def kernel(
    sizes, sol_in, res_in, dir_in, img_in, gram_in, sol_out, res_out, dir_out,
    sol, res, prev, prev_img, gram, land, strip, halo, done, back, part, parts, early, earlies,
    local_sem, send_sem, recv_sem,
):
    ngx, ngy, ngz, n, lx, lz, width = sizes
    s, level = lx * lz, ngz // 2
    per = n // (ngx * level)
    some = per * s
    gx, gy, gz = lax.axis_index("gx"), lax.axis_index("gy"), lax.axis_index("gz")
    column = gx * ngz + gz
    place = gy * n + column
    everyone = n * ngy

    loads = [
        pltpu.make_async_copy(a, b, local_sem.at[i])
        for i, (a, b) in enumerate(
            ((res_in, res), (gram_in, gram), (dir_in, prev), (img_in, prev_img), (sol_in, sol))
        )
    ]
    for load in loads:
        load.start()

    low = gz < level
    floors = [
        jnp.where(
            low,
            jnp.where(ngz - 1 - k > gz, ngz - 1 - k, ngz - 2 - k),
            jnp.where(k < gz, k, k + 1),
        )
        for k in range(ngz - 1)
    ] + [gz]
    chip = gx - jnp.bitwise_and(gx, 1)
    across = [jnp.bitwise_xor(chip, dx) for dx in range(ngx)]
    ways = sorted(
        ((dx, dy, k) for dx in range(ngx) for dy in range(ngy) for k in range(ngz)),
        key=lambda way: (way[2] >= level, way[0] % 2, -way[1], way[2] - (way[0] > 1)),
    )
    ways.remove((0, 0, ngz - 1))
    flock = []
    for dx, dy, k in ways:
        if True:
            ox, oy, oz = across[dx], 1 - gy if dy else gy, floors[k]
            if (dx, dy, k) == (1, 0, ngz - 1):
                ox = jnp.bitwise_xor(gx, 1)
            into = ox * level + jnp.bitwise_and(oz, level - 1)
            flock.append((dy == 0, k >= level, into, ox * ngz + oz, {"gx": ox, "gy": oy, "gz": oz}))
    owner = gx * level + jnp.bitwise_and(gz, level - 1)

    def remote(source, target, sent, arrived, where):
        pltpu.make_async_remote_copy(
            src_ref=source, dst_ref=target, send_sem=send_sem.at[sent], recv_sem=recv_sem.at[arrived],
            device_id=where, device_id_type=MESH,
        ).start()

    def wait(ref, semaphore):
        pltpu.make_async_copy(ref, ref, semaphore).wait()

    land[...] = jnp.zeros_like(land)
    barrier = pltpu.get_barrier_semaphore()
    for _, peer in sorted(zip(ways, flock), key=lambda pair: pair[0][2] - (pair[0][0] > 1) - pair[0][1]):
        pl.semaphore_signal(barrier, inc=1, device_id=peer[4], device_id_type=MESH)
    loads[0].wait()
    depth = width // s
    lanes = lax.broadcasted_iota(jnp.int32, (n, width), 1)
    packed = jnp.zeros((n, width), jnp.float32)
    for i in range(s):
        line = res[pl.ds(i, n, stride=s), :]
        line = pltpu.roll(line, lax.rem(i * depth + jnp.where(gy == 0, depth, 0), width), 1)
        packed = jnp.where(lanes // depth == i, line, packed)
    for i in range(n):
        strip[i] = packed[i : i + 1, :]
    pl.semaphore_wait(barrier, everyone - 1)

    mine = land.at[pl.ds(column * some, some), :]
    spans = spans_of(ngz, lx, lz)

    def by_plane(work):
        for span in sorted(set(spans)):
            here = functools.reduce(jnp.logical_or, [gz == g for g in range(ngz) if spans[g] == span])
            pl.when(here)(functools.partial(work, *span))

    def edge(into, where):
        remote(strip.at[pl.ds(into * per, per)], halo.at[pl.ds(column * per, per)], 5, 1, where)

    def cross(begin, end):
        for same, level_with, into, _, where in flock:
            if not level_with and not same:
                edge(into, where)
            elif not level_with:
                remote(
                    res.reshape(n, s, width).at[pl.ds(into * per, per), pl.ds(begin, end - begin), :],
                    land.reshape(per * n, s, width).at[pl.ds(column * per, per), pl.ds(begin, end - begin), :],
                    6, 8, where,
                )

    by_plane(cross)
    for same, level_with, into, _, where in flock:
        if level_with and same:
            remote(res.at[pl.ds(into * some, some), :], mine, 0, 0, where)
        elif level_with:
            edge(into, where)
    pltpu.make_async_copy(res.at[pl.ds(owner * some, some), :], mine, recv_sem.at[0]).start()

    def flat(ref, first, stride):
        return jnp.concatenate([ref[pl.ds(first + i, n, stride=stride), :] for i in range(s)], axis=1)

    def send_all(source, target, sent, arrived):
        for peer in flock:
            remote(source, target, sent, arrived, peer[4])
        pltpu.make_async_copy(source, target, recv_sem.at[arrived]).start()

    planes = [(x, z) for x in range(lx) for z in range(lz)]
    for load in loads[1:4]:
        load.wait()
    p, q = flat(prev, 0, s), flat(prev_img, 0, s)
    q_parts = parts_of(q)
    early[0] = pack(gram_of(parts_of(p), q_parts))
    eye = (lax.broadcasted_iota(jnp.int32, (n, n), 0) == lax.broadcasted_iota(jnp.int32, (n, n), 1)).astype(jnp.float32)
    inverse = eliminate(0.5 * (gram[...] + gram[...].T), eye)

    wait(land.at[pl.ds(0, level * ngx * some), :], recv_sem.at[0])
    above = ngx * per * sum(end - begin for begin, end in spans[level:])
    below = ngx * per * sum(end - begin for begin, end in spans[:level])

    @pl.when(low)
    def _():
        wait(land.at[pl.ds(0, above), :], recv_sem.at[8])

    @pl.when(jnp.logical_not(low))
    def _():
        wait(land.at[pl.ds(0, below), :], recv_sem.at[8])


    lines = {(x, z): [land[pl.ds(a * s + x * lz + z, n, stride=some), :] for a in range(per)] for x, z in planes}
    sweeps = [
        smooth([[lines[x, z][a] for z in range(lz)] for x in range(lx)], ngx, ngz, gy, True) for a in range(per)
    ]
    begun = [[next(sweep) for _ in range(2)] for sweep in sweeps]
    wait(halo, recv_sem.at[1])
    beyond = [jnp.concatenate([halo[i * per + a] for i in range(n)], axis=0) for a in range(per)]
    zone = width // per
    outer = jnp.where(gy == 0, zone - depth, 0)
    shift = jnp.where(gy == 0, zone, depth)

    def border_of(x, z):
        i = x * lz + z
        edge = None
        for a in range(per):
            begin = a * zone
            inside = pltpu.roll(lines[x, z][a], lax.rem(begin + shift + jnp.where(gy == 0, width - depth, 0), width), 1)
            outside = pltpu.roll(beyond[a], lax.rem(begin + outer + width - i * depth, width), 1)
            at = lanes - (begin + outer)
            value = jnp.where(jnp.logical_and(at >= 0, at < depth), outside, inside)
            edge = value if edge is None else jnp.where(lanes >= begin, value, edge)
        return edge

    border = jnp.where(gy == 0, width - depth, 0)
    at_border = jnp.logical_and(lanes >= border, lanes < border + depth)

    def keep(field, values, odd=None):
        for i, (x, z) in enumerate(planes):
            if odd is not None and x % 2 != odd:
                continue
            edge = values[per][x, z]
            for a in range(per):
                back_shift = lax.rem(2 * width - a * zone - shift - jnp.where(gy == 0, width - depth, 0), width)
                value = jnp.where(at_border, pltpu.roll(edge, back_shift, 1), values[a][x, z])
                done[field, pl.ds(a * s + i, n, stride=some), :] = value
        source, target = (ref.at[field].reshape(ref.shape[1] // s, s, width) for ref in (done, back))
        rows = pl.ds(0, s) if odd is None else pl.ds(odd * (s // 2), s // 2)
        target = target.at[pl.ds(owner * per, per), rows, :]
        for same, level_with, _, home, where in flock:
            if same and level_with:
                remote(source.at[pl.ds(home * per, per), rows, :], target, 1, 2 + field, where)
        pltpu.make_async_copy(source.at[pl.ds(column * per, per), rows, :], target, recv_sem.at[2 + field]).start()

    edge_rows = [[border_of(x, z) for z in range(lz)] for x in range(lx)]
    sweeps.append(smooth(edge_rows, ngx, ngz, gy, False))
    begun.append([])
    for step in range(8):
        found = [past[step] if step < len(past) else next(sweep) for past, sweep in zip(begun, sweeps)]
        if step in (1, 3):
            keep(0, [forward for forward, _ in found], step // 2)
        if step in (4, 6):
            keep(1, [state for _, state in found], 1 if step == 4 else 0)
    keep(2, [image for image, _ in found])
    send_all(early.at[0], earlies.at[0, place], 2, 5)

    wait(back.at[0], recv_sem.at[2])
    yf = flat(back.at[0], 0, s)
    y_parts = parts_of(yf)
    early[1] = pack(26.0 * gram_of(y_parts, y_parts))
    send_all(early.at[1], earlies.at[1, place], 3, 6)

    wait(back.at[1], recv_sem.at[3])
    zf = flat(back.at[1], 0, s)
    uf = zf - yf
    u_parts = parts_of(uf)
    part[...] = pack(jnp.concatenate([gram_of(u_parts, u_parts), gram_of(parts_of(zf), q_parts)], axis=1))
    send_all(part, parts.at[place], 4, 7)

    def summed(ref):
        return tree_sum([ref[i] for i in range(everyone)])

    wait(earlies.at[0], recv_sem.at[5])
    middle = dot(dot(inverse, unpack(summed(earlies.at[0]), n)), inverse)
    pair_parts = parts_of(jnp.concatenate([inverse, middle], axis=0))
    wait(earlies.at[1], recv_sem.at[6])
    gram_zr = unpack(summed(earlies.at[1]), n)
    zr_parts = parts_of(gram_zr)
    found = product(pair_parts, zr_parts, ((1,), (0,)))
    beta, inner = found[:n], found[n:]
    known = gram_zr + product(zr_parts, parts_of(inner), ((1,), (0,)))
    blocks = 128 // (2 * n)
    right_parts = parts_of(jnp.concatenate([-26.0 * eye, beta] * blocks, axis=0))
    left_parts = parts_of(jnp.concatenate([0.0 * eye, beta] * blocks, axis=0).T)
    row, lane = (lax.broadcasted_iota(jnp.int32, (n, 128), i) for i in range(2))
    mine_only = row // (n // blocks) == lane // (2 * n)
    mixed = wide(beta, parts_of(jnp.concatenate([p, q], axis=1)))
    direction = zf + mixed[:, : s * width]
    wait(back.at[2], recv_sem.at[4])
    wf = flat(back.at[2], 0, s)
    both = jnp.concatenate([direction, wf + mixed[:, s * width :]], axis=1)
    both_parts = parts_of(both)
    for i in range(s):
        dir_out[pl.ds(i, n, stride=s), :] = direction[:, i * width : (i + 1) * width]
    loads[4].wait()
    wait(land.at[pl.ds(0, (level * ngx - 1) * some), :], send_sem.at[0])
    by_plane(lambda begin, end: wait(land.at[pl.ds(0, level * ngx * per * (end - begin)), :], send_sem.at[6]))
    wait(halo, send_sem.at[5])
    wait(back.at[pl.ds(0, 3), pl.ds(0, (n // per - 1) * some), :], send_sem.at[1])
    wait(earlies.at[0, pl.ds(0, everyone - 1)], send_sem.at[2])
    wait(earlies.at[1, pl.ds(0, everyone - 1)], send_sem.at[3])

    wait(parts, recv_sem.at[7])
    total = parts_of(jnp.where(mine_only, jnp.concatenate([summed(parts)] * blocks, axis=0), 0.0))
    curvature = known + product(total, right_parts, ((1,), (0,))) + gram_of(left_parts, total)
    alpha = eliminate(curvature, gram_zr)
    step = wide(alpha, both_parts)
    for i in range(s):
        rows = pl.ds(i, n, stride=s)
        sol_out[rows, :] = sol[rows, :] + step[:, i * width : (i + 1) * width]
        res_out[rows, :] = res[rows, :] - step[:, (s + i) * width : (s + i + 1) * width]
    wait(parts.at[pl.ds(0, everyone - 1)], send_sem.at[4])


def write(*refs):
    *arrays, size, semaphore = refs
    half = len(arrays) // 2
    for source, target in zip(arrays[:half], arrays[half:]):
        pltpu.make_async_copy(source, target, semaphore).start()
    pltpu.make_async_copy(size, size, semaphore).wait()


def whole_body(sizes, *args):
    ngx, ngy, ngz, n, lx, lz, width = sizes
    s, everyone = lx * lz, n * ngy
    rows = n * s
    shape = args[0].shape
    field = jax.ShapeDtypeStruct((rows, width), jnp.float32)
    anywhere = pl.BlockSpec(memory_space=pl.ANY)
    inside = pl.BlockSpec(memory_space=pltpu.VMEM)
    block = pltpu.VMEM((rows, width), jnp.float32)
    per = 2 * n // (ngx * ngz)
    packed = n * n // 128
    outs = pl.pallas_call(
        functools.partial(kernel, sizes),
        out_shape=(block,) * 3,
        in_specs=[anywhere] * 5,
        out_specs=[inside] * 3,
        scratch_shapes=[
            block, block, block, block,
            pltpu.VMEM((n, n), jnp.float32),
            pltpu.VMEM((per * rows, width), jnp.float32),
            pltpu.VMEM((n, 1, width), jnp.float32),
            pltpu.VMEM((per * n, 1, width), jnp.float32),
            pltpu.VMEM((3, per * rows, width), jnp.float32),
            pltpu.VMEM((3, rows, width), jnp.float32),
            pltpu.VMEM((2 * packed, 128), jnp.float32),
            pltpu.VMEM((everyone, 2 * packed, 128), jnp.float32),
            pltpu.VMEM((2, packed, 128), jnp.float32),
            pltpu.VMEM((2, everyone, packed, 128), jnp.float32),
            pltpu.SemaphoreType.DMA((5,)),
            pltpu.SemaphoreType.DMA((7,)),
            pltpu.SemaphoreType.DMA((9,)),
        ],
        compiler_params=pltpu.CompilerParams(
            collective_id=0, has_side_effects=True
        ),
    )(*(a.reshape(rows, width) for a in args[:4]), args[4])
    outs = [pltpu.with_memory_space_constraint(a, pltpu.VMEM) for a in outs]
    outs = pl.pallas_call(
        write,
        out_shape=(field,) * 3,
        in_specs=[inside] * 3,
        out_specs=[anywhere] * 3,
        scratch_shapes=[pltpu.VMEM((3 * rows, width), jnp.float32), pltpu.SemaphoreType.DMA],

    )(*outs)
    return tuple(a.reshape(shape) for a in outs)


def pick_body(mesh, solution, residual, direction_prev, image_prev, gram_prev):
    ngx, ngy, ngz = (mesh.shape[axis] for axis in ("gx", "gy", "gz"))
    n, lx, lz, width = residual.shape
    fits = n == ngx * ngz and lx == 2 and lz % 2 == 0 and (lx * lz) % 8 == 0
    fits = fits and width % 128 == 0 and n % 16 == 0 and 128 % (2 * n) == 0 and ngy == 2 and ngz > 1 and width >= 4 * (width // (lx * lz)) and (ngx & (ngx - 1)) == 0 and (ngz & (ngz - 1)) == 0 and width % (lx * lz) == 0 and width // (lx * lz) >= 15
    args = (solution, residual, direction_prev, image_prev, gram_prev)
    if fits:
        return whole_body((ngx, ngy, ngz, n, lx, lz, width), *args)
    return body(*args)


def solution(mesh):
    in_specs = (
        P(None, "gx", "gz", "gy"),
        P(None, "gx", "gz", "gy"),
        P(None, "gx", "gz", "gy"),
        P(None, "gx", "gz", "gy"),
        P(),
    )
    out_specs = (P(None, "gx", "gz", "gy"), P(None, "gx", "gz", "gy"), P(None, "gx", "gz", "gy"))
    return jax.shard_map(functools.partial(pick_body, mesh), mesh=mesh, in_specs=in_specs, out_specs=out_specs, check_vma=False)
```

```python
import functools

import jax
import jax.numpy as jnp
from jax import lax
from jax.experimental import pallas as pl
from jax.experimental.pallas import tpu as pltpu
from jax.sharding import PartitionSpec as P


def with_halo(value, sides, width):
    for axis, dim in sides:
        devices, length = (lax.axis_size(axis), value.shape[dim])
        up = [(i, (i + 1) % devices) for i in range(devices - 1)]
        down = [(j, i) for i, j in up]
        last = lax.slice_in_dim(value, length - width, length, axis=dim)
        first = lax.slice_in_dim(value, 0, width, axis=dim)
        before = lax.ppermute(last, axis, up)
        after = lax.ppermute(first, axis, down)
        value = jnp.concatenate([before, value, after], axis=dim)
    return value


def box_sum(padded):
    total = padded[:, :-2] + padded[:, 1:-1] + padded[:, 2:]
    total = total[:, :, :-2] + total[:, :, 1:-1] + total[:, :, 2:]
    return total[:, :, :, :-2] + total[:, :, :, 1:-1] + total[:, :, :, 2:]


def colors_of(shape):
    first = lax.broadcasted_iota(jnp.int32, shape, 1) % 2
    second = lax.broadcasted_iota(jnp.int32, shape, 2) % 2
    third = lax.broadcasted_iota(jnp.int32, shape, 3) % 2
    return 4 * first + 2 * second + third


def local_gram(left, right):
    return jnp.einsum("kxzy,lxzy->kl", left, right, precision=lax.Precision.HIGHEST)


def combine(field, mixing):
    return jnp.einsum("kxzy,kl->lxzy", field, mixing, precision=lax.Precision.HIGHEST)


def small_dot(left, right):
    return jnp.dot(left, right, precision=lax.Precision.HIGHEST)


def spd_solve(matrix, target):
    order = matrix.shape[0]
    sym = 0.5 * (matrix + matrix.T)
    lower = jnp.zeros_like(sym)
    for col in range(order):
        column = sym[col:, col] - jnp.sum(lower[col:, :col] * lower[col, :col][None, :], axis=1)
        pivot = jnp.sqrt(column[0])
        lower = lower.at[col:, col].set(column / pivot)
    middle = jnp.zeros_like(target)
    for row in range(order):
        value = target[row] - jnp.sum(lower[row, :row][:, None] * middle[:row], axis=0)
        middle = middle.at[row].set(value / lower[row, row])
    answer = jnp.zeros_like(target)
    for row in range(order - 1, -1, -1):
        value = middle[row] - jnp.sum(lower[row + 1 :, row][:, None] * answer[row + 1 :], axis=0)
        answer = answer.at[row].set(value / lower[row, row])
    return answer


def sweep_box(field):
    padded = with_halo(field, (("gx", 1), ("gy", 3), ("gz", 2)), 1)
    return box_sum(padded)


def body(solution, residual, direction_prev, image_prev, gram_prev):
    colors = colors_of(residual.shape)
    smoothed = jnp.where(colors == 0, residual / 26.0, jnp.float32(0.0))
    for shade in list(range(1, 8)) + list(range(6, -1, -1)):
        boxed = sweep_box(smoothed)
        smoothed = jnp.where(colors == shade, (residual + boxed - smoothed) / 26.0, smoothed)
    padded = with_halo(smoothed, (("gx", 1), ("gy", 3), ("gz", 2)), 1)
    image = 27.0 * smoothed - box_sum(padded)
    sums = (
        local_gram(smoothed, residual),
        local_gram(smoothed, image),
        local_gram(smoothed, image_prev),
        local_gram(direction_prev, image),
        local_gram(direction_prev, image_prev),
    )
    gram_zr, gram_zw, gram_zq, gram_pw, gram_pq = lax.psum(
        (sums[0], sums[1], sums[2], sums[3], sums[4]), ("gx", "gy", "gz")
    )
    beta_mix = spd_solve(gram_prev, gram_zr)
    direction = smoothed + combine(direction_prev, beta_mix)
    image_new = image + combine(image_prev, beta_mix)
    curvature = gram_zw + small_dot(gram_zq, beta_mix) + small_dot(beta_mix.T, gram_pw)
    curvature = curvature + small_dot(small_dot(beta_mix.T, gram_pq), beta_mix)
    alpha_step = spd_solve(curvature, gram_zr)
    solution_new = solution + combine(direction, alpha_step)
    residual_new = residual - combine(image_new, alpha_step)
    return (solution_new, residual_new, direction)


MESH = pl.DeviceIdType.MESH
HIGHEST = lax.Precision.HIGHEST


def dot(left, right):
    return jnp.dot(left, right, precision=HIGHEST, preferred_element_type=jnp.float32)


def dot_nt(left, right):
    return lax.dot_general(
        left, right, (((1,), (1,)), ((), ())), precision=HIGHEST, preferred_element_type=jnp.float32
    )


def parts_of(value):
    first = value.astype(jnp.bfloat16)
    rest = value - first.astype(jnp.float32)
    second = rest.astype(jnp.bfloat16)
    third = (rest - second.astype(jnp.float32)).astype(jnp.bfloat16)
    return first, second, third


def product(left, right, contract):
    order = left[0].shape[0]
    total = None
    for i, term in enumerate(right):
        stack = jnp.concatenate(left[: 3 - i], axis=0) if i < 2 else left[0]
        out = lax.dot_general(stack, term, (contract, ((), ())), preferred_element_type=jnp.float32)
        for j in range(3 - i):
            piece = out[j * order : (j + 1) * order]
            total = piece if total is None else total + piece
    return total


def gram_of(left, right):
    return product(left, right, ((1,), (1,)))


def small(left, right):
    return product(parts_of(left), parts_of(right), ((1,), (0,)))


def wide(turned, right):
    a, b, c = (v.astype(jnp.float32) for v in parts_of(turned))
    d, e, f = right
    left = jnp.concatenate([a, a, b, b, a, c], axis=0).T.astype(jnp.bfloat16)
    return jnp.dot(left, jnp.concatenate([d, e, d, e, f, d], axis=0), preferred_element_type=jnp.float32)


def eliminate(matrix, target):
    order = matrix.shape[0]
    rows = lax.broadcasted_iota(jnp.int32, matrix.shape, 0)
    columns = [jnp.broadcast_to(matrix[:, k : k + 1], matrix.shape) for k in range(order)]
    scale = jnp.zeros(matrix.shape, jnp.float32)
    for c in range(order):
        inverse = 1.0 / columns[c][c : c + 1, :]
        here = rows == c
        factor = jnp.where(here, 0.0, columns[c] * inverse)
        for k in range(c + 1, order):
            columns[k] = columns[k] - factor * columns[k][c : c + 1, :]
        target = target - factor * target[c : c + 1, :]
        scale = jnp.where(here, inverse, scale)
    return target * scale


def smooth(res, ngx, ngz, gy, ends):
    lx, lz = len(res), len(res[0])
    count, ny = res[0][0].shape
    row = lax.broadcasted_iota(jnp.int32, (count, ny), 0)
    lane = lax.broadcasted_iota(jnp.int32, (count, ny), 1)
    even = lane % 2 == 0
    edges = {
        "xp": (row < ngz, ngz),
        "xn": (row >= (ngx - 1) * ngz, count - ngz),
        "zp": (row % ngz == 0, 1),
        "zn": (row % ngz == ngz - 1, count - 1),
    }
    odd = jnp.logical_not(even)
    if ends:
        first, last = jnp.where(gy == 0, 0, -8), jnp.where(gy == 0, -8, ny - 1)
        cut = jnp.where(gy == 0, ny - 3, 0)
        valid = jnp.logical_or(lane < cut, lane > cut + 2)
        valid_even, valid_odd = jnp.logical_and(valid, even), jnp.logical_and(valid, odd)
        twice = 2.0 - jnp.where(jnp.logical_or(lane == first, lane == last), 1.0, 0.0)
        below = 3.0 - jnp.where(jnp.logical_or(lane == first + 1, lane == last), 1.0, 0.0)
        above = 3.0 - jnp.where(jnp.logical_or(lane == last - 1, lane == first), 1.0, 0.0)
    else:
        twice, below, above = jnp.float32(2.0), jnp.float32(3.0), jnp.float32(3.0)
    zero = jnp.zeros((count, ny), jnp.float32)
    memo = {}

    def moved(value, kind):
        if value is None:
            return None
        key = (kind, id(value))
        if key not in memo:
            edge, amount = edges[kind]
            memo[key] = (value, jnp.where(edge, zero, pltpu.roll(value, amount, 0)))
        return memo[key][1]

    def add(*values):
        total = None
        for value in values:
            if value is not None:
                total = value if total is None else total + value
        return total

    state = {(x, z): None for x in range(lx) for z in range(lz)}

    def z_pair(x, z):
        before = state[x, z - 1] if z > 0 else moved(state[x, lz - 1], "zp")
        after = state[x, z + 1] if z < lz - 1 else moved(state[x, 0], "zn")
        return add(before, after)

    def neighbours(x, z):
        def line(other):
            return add(state[other, z], z_pair(other, z))

        before = line(x - 1) if x > 0 else moved_line(lx - 1, z, "xp")
        after = line(x + 1) if x < lx - 1 else moved_line(0, z, "xn")
        return add(z_pair(x, z), before, after)

    def moved_line(x, z, kind):
        return moved(add(state[x, z], z_pair(x, z)), kind)

    def woven(at_even, at_odd):
        if not ends:
            return jnp.where(even, at_even, at_odd)
        return jnp.where(valid_even, at_even, jnp.where(valid_odd, at_odd, zero))

    def shifted(value, k):
        return pltpu.roll(value, k, 1), pltpu.roll(value, ny - k, 1)

    def once(value):
        return sum(shifted(value, 1))

    def two(value):
        return sum(shifted(value, 2)) + twice * value

    third = jnp.float32(1.0 / 26.0)
    plan = [(0, 0), (0, 1), (1, 0), (1, 1), (1, 0), (0, 1), (0, 0)]
    forward = {}
    for step, (xp, zp) in enumerate(plan):
        fresh = {}
        for x in range(xp, lx, 2):
            for z in range(zp, lz, 2):
                near, value = neighbours(x, z), state[x, z]
                own = res[x][z]
                both = own if near is None else own + near
                share = third * both
                if value is None and near is None:
                    fresh[x, z] = jnp.where(even, share, third * (own + once(woven(share, zero))))
                    forward[x, z] = fresh[x, z]
                elif value is None:
                    mix = woven(near + share, near)
                    down, up = shifted(mix, 1)
                    pair, far = down + up, two(mix)
                    base = both + pair
                    later = third * (base + third * far)
                    fresh[x, z] = forward[x, z] = jnp.where(even, third * base, later)
                    if step == 3:
                        deep = sum(shifted(mix, 3)) + below * down + above * up
                        again = base + third * (once(woven(zero, both)) + far + third * deep)
                        fresh[x, z] = jnp.where(even, third * again, later)
                else:
                    mix = woven(near + value, near + share)
                    base = both + once(mix)
                    fresh[x, z] = third * jnp.where(even, base + third * two(mix), base)
        state.update(fresh)
        yield forward, state
    image = {}
    for x in range(lx):
        for z in range(lz):
            box = add(state[x, z], neighbours(x, z))
            image[x, z] = 27.0 * state[x, z] - (box + once(jnp.where(valid, box, zero) if ends else box))
    yield image, None


def pack(value):
    rows = value.shape[0] * value.shape[1] // 128
    return jnp.concatenate([value[i : i + rows] for i in range(0, value.shape[0], rows)], axis=1)


def unpack(value, lanes):
    return jnp.concatenate([value[:, i : i + lanes] for i in range(0, value.shape[1], lanes)], axis=0)


def tree_sum(values):
    while len(values) > 1:
        values = [sum(values[i + 1 : i + 2], values[i]) for i in range(0, len(values), 2)]
    return values[0]


def spans_of(ngz, lx, lz):
    level, spans = ngz // 2, []
    for plane in range(ngz):
        rows = []
        for x in range(lx):
            for z in range(lz):
                below = level * lz - 1 - (plane * lz + z)
                away, reach = (below, 5) if below >= 0 else (-1 - below, 6)
                if away <= reach - 2 * (x % 2):
                    rows.append(x * lz + z)
        spans.append((rows[0], rows[-1] + 1) if rows else (0, 0))
    return spans


def kernel(
    sizes, sol_in, res_in, dir_in, img_in, gram_in, sol_out, res_out, dir_out,
    sol, res, prev, prev_img, gram, land, strip, halo, done, back, part, parts, early, earlies,
    local_sem, send_sem, recv_sem,
):
    ngx, ngy, ngz, n, lx, lz, width = sizes
    s, level = lx * lz, ngz // 2
    per = n // (ngx * level)
    some = per * s
    gx, gy, gz = lax.axis_index("gx"), lax.axis_index("gy"), lax.axis_index("gz")
    column = gx * ngz + gz
    place = gy * n + column
    everyone = n * ngy

    loads = [
        pltpu.make_async_copy(a, b, local_sem.at[i])
        for i, (a, b) in enumerate(
            ((res_in, res), (gram_in, gram), (dir_in, prev), (img_in, prev_img), (sol_in, sol))
        )
    ]
    for load in loads:
        load.start()

    low = gz < level
    floors = [
        jnp.where(
            low,
            jnp.where(ngz - 1 - k > gz, ngz - 1 - k, ngz - 2 - k),
            jnp.where(k < gz, k, k + 1),
        )
        for k in range(ngz - 1)
    ] + [gz]
    chip = gx - jnp.bitwise_and(gx, 1)
    across = [jnp.bitwise_xor(chip, dx) for dx in range(ngx)]
    ways = sorted(
        ((dx, dy, k) for dx in range(ngx) for dy in range(ngy) for k in range(ngz)),
        key=lambda way: (way[2] >= level, way[0] % 2, -way[1], way[2] - (way[0] > 1)),
    )
    ways.remove((0, 0, ngz - 1))
    flock = []
    for dx, dy, k in ways:
        if True:
            ox, oy, oz = across[dx], 1 - gy if dy else gy, floors[k]
            if (dx, dy, k) == (1, 0, ngz - 1):
                ox = jnp.bitwise_xor(gx, 1)
            into = ox * level + jnp.bitwise_and(oz, level - 1)
            flock.append((dy == 0, k >= level, into, ox * ngz + oz, {"gx": ox, "gy": oy, "gz": oz}))
    owner = gx * level + jnp.bitwise_and(gz, level - 1)

    def remote(source, target, sent, arrived, where):
        pltpu.make_async_remote_copy(
            src_ref=source, dst_ref=target, send_sem=send_sem.at[sent], recv_sem=recv_sem.at[arrived],
            device_id=where, device_id_type=MESH,
        ).start()

    def wait(ref, semaphore):
        pltpu.make_async_copy(ref, ref, semaphore).wait()

    land[...] = jnp.zeros_like(land)
    barrier = pltpu.get_barrier_semaphore()
    for _, peer in sorted(zip(ways, flock), key=lambda pair: pair[0][2] - (pair[0][0] > 1) - pair[0][1]):
        pl.semaphore_signal(barrier, inc=1, device_id=peer[4], device_id_type=MESH)
    loads[0].wait()
    depth = width // s
    lanes = lax.broadcasted_iota(jnp.int32, (n, width), 1)
    packed = jnp.zeros((n, width), jnp.float32)
    for i in range(s):
        line = res[pl.ds(i, n, stride=s), :]
        line = pltpu.roll(line, lax.rem(i * depth + jnp.where(gy == 0, depth, 0), width), 1)
        packed = jnp.where(lanes // depth == i, line, packed)
    for i in range(n):
        strip[i] = packed[i : i + 1, :]
    pl.semaphore_wait(barrier, everyone - 1)

    mine = land.at[pl.ds(column * some, some), :]
    spans = spans_of(ngz, lx, lz)

    def by_plane(work):
        for span in sorted(set(spans)):
            here = functools.reduce(jnp.logical_or, [gz == g for g in range(ngz) if spans[g] == span])
            pl.when(here)(functools.partial(work, *span))

    def edge(into, where):
        remote(strip.at[pl.ds(into * per, per)], halo.at[pl.ds(column * per, per)], 0, 1, where)

    def cross(begin, end):
        for same, level_with, into, _, where in flock:
            if not level_with and not same:
                edge(into, where)
            elif not level_with:
                remote(
                    res.reshape(n, s, width).at[pl.ds(into * per, per), pl.ds(begin, end - begin), :],
                    land.reshape(per * n, s, width).at[pl.ds(column * per, per), pl.ds(begin, end - begin), :],
                    1, 8, where,
                )

    by_plane(cross)
    for same, level_with, into, _, where in flock:
        if level_with and same:
            remote(res.at[pl.ds(into * some, some), :], mine, 0, 0, where)
        elif level_with:
            edge(into, where)
    pltpu.make_async_copy(res.at[pl.ds(owner * some, some), :], mine, recv_sem.at[0]).start()

    def flat(ref, first, stride):
        return jnp.concatenate([ref[pl.ds(first + i, n, stride=stride), :] for i in range(s)], axis=1)

    def send_all(source, target, sent, arrived):
        for peer in flock:
            remote(source, target, sent, arrived, peer[4])
        pltpu.make_async_copy(source, target, recv_sem.at[arrived]).start()

    planes = [(x, z) for x in range(lx) for z in range(lz)]
    for load in loads[1:4]:
        load.wait()
    p, q = flat(prev, 0, s), flat(prev_img, 0, s)
    q_parts = parts_of(q)
    early[0] = pack(gram_of(parts_of(p), q_parts))
    eye = (lax.broadcasted_iota(jnp.int32, (n, n), 0) == lax.broadcasted_iota(jnp.int32, (n, n), 1)).astype(jnp.float32)
    inverse = eliminate(0.5 * (gram[...] + gram[...].T), eye)

    wait(land.at[pl.ds(0, level * ngx * some), :], recv_sem.at[0])
    above = ngx * per * sum(end - begin for begin, end in spans[level:])
    below = ngx * per * sum(end - begin for begin, end in spans[:level])

    @pl.when(low)
    def _():
        wait(land.at[pl.ds(0, above), :], recv_sem.at[8])

    @pl.when(jnp.logical_not(low))
    def _():
        wait(land.at[pl.ds(0, below), :], recv_sem.at[8])


    lines = {(x, z): [land[pl.ds(a * s + x * lz + z, n, stride=some), :] for a in range(per)] for x, z in planes}
    sweeps = [
        smooth([[lines[x, z][a] for z in range(lz)] for x in range(lx)], ngx, ngz, gy, True) for a in range(per)
    ]
    begun = [[next(sweep) for _ in range(2)] for sweep in sweeps]
    wait(halo, recv_sem.at[1])
    beyond = [jnp.concatenate([halo[i * per + a] for i in range(n)], axis=0) for a in range(per)]
    zone = width // per
    outer = jnp.where(gy == 0, zone - depth, 0)
    shift = jnp.where(gy == 0, zone, depth)

    def border_of(x, z):
        i = x * lz + z
        edge = None
        for a in range(per):
            begin = a * zone
            inside = pltpu.roll(lines[x, z][a], lax.rem(begin + shift + jnp.where(gy == 0, width - depth, 0), width), 1)
            outside = pltpu.roll(beyond[a], lax.rem(begin + outer + width - i * depth, width), 1)
            at = lanes - (begin + outer)
            value = jnp.where(jnp.logical_and(at >= 0, at < depth), outside, inside)
            edge = value if edge is None else jnp.where(lanes >= begin, value, edge)
        return edge

    border = jnp.where(gy == 0, width - depth, 0)
    at_border = jnp.logical_and(lanes >= border, lanes < border + depth)

    def keep(field, values, odd=None):
        for i, (x, z) in enumerate(planes):
            if odd is not None and x % 2 != odd:
                continue
            edge = values[per][x, z]
            for a in range(per):
                back_shift = lax.rem(2 * width - a * zone - shift - jnp.where(gy == 0, width - depth, 0), width)
                value = jnp.where(at_border, pltpu.roll(edge, back_shift, 1), values[a][x, z])
                done[field, pl.ds(a * s + i, n, stride=some), :] = value
        source, target = (ref.at[field].reshape(ref.shape[1] // s, s, width) for ref in (done, back))
        rows = pl.ds(0, s) if odd is None else pl.ds(odd * (s // 2), s // 2)
        target = target.at[pl.ds(owner * per, per), rows, :]
        for same, level_with, _, home, where in flock:
            if same and level_with:
                remote(source.at[pl.ds(home * per, per), rows, :], target, 0, 2 + field, where)
        pltpu.make_async_copy(source.at[pl.ds(column * per, per), rows, :], target, recv_sem.at[2 + field]).start()

    edge_rows = [[border_of(x, z) for z in range(lz)] for x in range(lx)]
    sweeps.append(smooth(edge_rows, ngx, ngz, gy, False))
    begun.append([])
    for step in range(8):
        found = [past[step] if step < len(past) else next(sweep) for past, sweep in zip(begun, sweeps)]
        if step in (1, 3):
            keep(0, [forward for forward, _ in found], step // 2)
        if step in (4, 6):
            keep(1, [state for _, state in found], 1 if step == 4 else 0)
    keep(2, [image for image, _ in found])
    send_all(early.at[0], earlies.at[0, place], 2, 5)

    wait(back.at[0], recv_sem.at[2])
    yf = flat(back.at[0], 0, s)
    y_parts = parts_of(yf)
    early[1] = pack(26.0 * gram_of(y_parts, y_parts))
    send_all(early.at[1], earlies.at[1, place], 2, 6)

    wait(back.at[1], recv_sem.at[3])
    zf = flat(back.at[1], 0, s)
    uf = zf - yf
    u_parts = parts_of(uf)
    part[...] = pack(jnp.concatenate([gram_of(u_parts, u_parts), gram_of(parts_of(zf), q_parts)], axis=1))
    send_all(part, parts.at[place], 3, 7)

    def summed(ref):
        return tree_sum([ref[i] for i in range(everyone)])

    wait(earlies.at[0], recv_sem.at[5])
    middle = dot(dot(inverse, unpack(summed(earlies.at[0]), n)), inverse)
    pair_parts = parts_of(jnp.concatenate([inverse, middle], axis=0))
    wait(earlies.at[1], recv_sem.at[6])
    gram_zr = unpack(summed(earlies.at[1]), n)
    zr_parts = parts_of(gram_zr)
    found = product(pair_parts, zr_parts, ((1,), (0,)))
    beta, inner = found[:n], found[n:]
    known = gram_zr + product(zr_parts, parts_of(inner), ((1,), (0,)))
    blocks = 128 // (2 * n)
    right_parts = parts_of(jnp.concatenate([-26.0 * eye, beta] * blocks, axis=0))
    left_parts = parts_of(jnp.concatenate([0.0 * eye, beta] * blocks, axis=0).T)
    row, lane = (lax.broadcasted_iota(jnp.int32, (n, 128), i) for i in range(2))
    mine_only = row // (n // blocks) == lane // (2 * n)
    mixed = wide(beta, parts_of(jnp.concatenate([p, q], axis=1)))
    direction = zf + mixed[:, : s * width]
    wait(back.at[2], recv_sem.at[4])
    wf = flat(back.at[2], 0, s)
    both = jnp.concatenate([direction, wf + mixed[:, s * width :]], axis=1)
    both_parts = parts_of(both)
    for i in range(s):
        dir_out[pl.ds(i, n, stride=s), :] = direction[:, i * width : (i + 1) * width]
    loads[4].wait()
    gone = (level * ngx - 1) * some + per * n + 3 * (n // per - 1) * some
    wait(done.reshape(3 * n * some, width).at[pl.ds(0, gone), :], send_sem.at[0])
    by_plane(lambda begin, end: wait(land.at[pl.ds(0, level * ngx * per * (end - begin)), :], send_sem.at[1]))
    wait(earlies.at[pl.ds(0, 2), pl.ds(0, everyone - 1)], send_sem.at[2])

    wait(parts, recv_sem.at[7])
    total = parts_of(jnp.where(mine_only, jnp.concatenate([summed(parts)] * blocks, axis=0), 0.0))
    curvature = known + product(total, right_parts, ((1,), (0,))) + gram_of(left_parts, total)
    alpha = eliminate(curvature, gram_zr)
    step = wide(alpha, both_parts)
    for i in range(s):
        rows = pl.ds(i, n, stride=s)
        sol_out[rows, :] = sol[rows, :] + step[:, i * width : (i + 1) * width]
        res_out[rows, :] = res[rows, :] - step[:, (s + i) * width : (s + i + 1) * width]
    wait(parts.at[pl.ds(0, everyone - 1)], send_sem.at[3])


def write(*refs):
    *arrays, size, semaphore = refs
    half = len(arrays) // 2
    for source, target in zip(arrays[:half], arrays[half:]):
        pltpu.make_async_copy(source, target, semaphore).start()
    pltpu.make_async_copy(size, size, semaphore).wait()


def whole_body(sizes, *args):
    ngx, ngy, ngz, n, lx, lz, width = sizes
    s, everyone = lx * lz, n * ngy
    rows = n * s
    shape = args[0].shape
    field = jax.ShapeDtypeStruct((rows, width), jnp.float32)
    anywhere = pl.BlockSpec(memory_space=pl.ANY)
    inside = pl.BlockSpec(memory_space=pltpu.VMEM)
    block = pltpu.VMEM((rows, width), jnp.float32)
    per = 2 * n // (ngx * ngz)
    packed = n * n // 128
    outs = pl.pallas_call(
        functools.partial(kernel, sizes),
        out_shape=(block,) * 3,
        in_specs=[anywhere] * 5,
        out_specs=[inside] * 3,
        scratch_shapes=[
            block, block, block, block,
            pltpu.VMEM((n, n), jnp.float32),
            pltpu.VMEM((per * rows, width), jnp.float32),
            pltpu.VMEM((n, 1, width), jnp.float32),
            pltpu.VMEM((per * n, 1, width), jnp.float32),
            pltpu.VMEM((3, per * rows, width), jnp.float32),
            pltpu.VMEM((3, rows, width), jnp.float32),
            pltpu.VMEM((2 * packed, 128), jnp.float32),
            pltpu.VMEM((everyone, 2 * packed, 128), jnp.float32),
            pltpu.VMEM((2, packed, 128), jnp.float32),
            pltpu.VMEM((2, everyone, packed, 128), jnp.float32),
            pltpu.SemaphoreType.DMA((5,)),
            pltpu.SemaphoreType.DMA((4,)),
            pltpu.SemaphoreType.DMA((9,)),
        ],
        compiler_params=pltpu.CompilerParams(
            collective_id=0, has_side_effects=True
        ),
    )(*(a.reshape(rows, width) for a in args[:4]), args[4])
    outs = [pltpu.with_memory_space_constraint(a, pltpu.VMEM) for a in outs]
    outs = pl.pallas_call(
        write,
        out_shape=(field,) * 3,
        in_specs=[inside] * 3,
        out_specs=[anywhere] * 3,
        scratch_shapes=[pltpu.VMEM((3 * rows, width), jnp.float32), pltpu.SemaphoreType.DMA],

    )(*outs)
    return tuple(a.reshape(shape) for a in outs)


def pick_body(mesh, solution, residual, direction_prev, image_prev, gram_prev):
    ngx, ngy, ngz = (mesh.shape[axis] for axis in ("gx", "gy", "gz"))
    n, lx, lz, width = residual.shape
    fits = n == ngx * ngz and lx == 2 and lz % 2 == 0 and (lx * lz) % 8 == 0
    fits = fits and width % 128 == 0 and n % 16 == 0 and 128 % (2 * n) == 0 and ngy == 2 and ngz > 1 and width >= 4 * (width // (lx * lz)) and (ngx & (ngx - 1)) == 0 and (ngz & (ngz - 1)) == 0 and width % (lx * lz) == 0 and width // (lx * lz) >= 15
    args = (solution, residual, direction_prev, image_prev, gram_prev)
    if fits:
        return whole_body((ngx, ngy, ngz, n, lx, lz, width), *args)
    return body(*args)


def solution(mesh):
    in_specs = (
        P(None, "gx", "gz", "gy"),
        P(None, "gx", "gz", "gy"),
        P(None, "gx", "gz", "gy"),
        P(None, "gx", "gz", "gy"),
        P(),
    )
    out_specs = (P(None, "gx", "gz", "gy"), P(None, "gx", "gz", "gy"), P(None, "gx", "gz", "gy"))
    return jax.shard_map(functools.partial(pick_body, mesh), mesh=mesh, in_specs=in_specs, out_specs=out_specs, check_vma=False)
```
